256 devices in a mesh: src: 16 (over x_hi, z), tgt: 16 (over x_lo, y, core).
Axes of the slice: x: 4 (x_hi: 2, x_lo: 2; x = x_hi * 2 + x_lo), y: 4, z: 8, core: 2. Of those that a mesh axis runs over, the one named last changes fastest.
Arguments:
- source_words: bfloat16 [32768, 300], P(('src', 'tgt')), may hold values from -3 to 3
- target_words: bfloat16 [30720, 300], P(('tgt', 'src')), may hold values from -24 to 24
Outputs:
- rotated: bfloat16 [32768, 300], P(('src', 'tgt'))
- matched: float32 [32768, 300], P(('src', 'tgt'))
- ortho: float32 [300, 300], replicated
- row_pot: float32 [32768], P(('src', 'tgt'))
- col_pot: float32 [30720], P(('tgt', 'src'))
The draws below stay inside these ranges and needn't reach their ends.
All inputs are finite; a program needn't handle non-finite values.
Results may differ from the reference program's by a relative error of at most 0.0034.
Values may be sent and summed in bfloat16 or wider, within the bound.
A program may use at most 64 MiB of HBM per device.

```python
import math
import jax
import jax.numpy as jnp
from jax import lax

D = 300
ITERS = 2
NEWTON = 12
NS = 32768
NT = 30720


def source_rows(key):
    base = jax.random.normal(jax.random.fold_in(key, 11), (NS, D), jnp.float32)
    ramp = jnp.exp(jnp.linspace(math.log(0.25), math.log(4.0), NS, dtype=jnp.float32))
    return jnp.clip(base * ramp[:, None], -3.0, 3.0)


def draw_source_words(key, part):
    return source_rows(key).astype(jnp.bfloat16)


def draw_target_words(key, part):
    base = jnp.clip(jax.random.normal(jax.random.fold_in(key, 23), (NT, D), jnp.float32), -3.0, 3.0)
    return base.astype(jnp.bfloat16)


def setup_inputs(seed: int = 0) -> dict:
    key_of = jax.random.split(jax.random.key(seed), 3)
    return {
        "source_words": draw_source_words(jax.random.fold_in(key_of[2], 71), 0),
        "target_words": draw_target_words(jax.random.fold_in(key_of[2], 71), 0),
    }


def row_lse(logits):
    top = lax.optimization_barrier(jnp.max(logits, axis=1))
    return top + jnp.log(lax.optimization_barrier(jnp.sum(jnp.exp(logits - top[:, None]), axis=1)))

def reference(source_words, target_words):
    scale = 4.0 / math.sqrt(D)
    block = math.gcd(NS, 512)
    count = NS // block
    blocks = source_words.reshape(count, block, D)
    highest = lax.Precision.HIGHEST

    def scores(rows_in):
        return jnp.dot(rows_in, target_words.T, preferred_element_type=jnp.float32) * scale
    col_pot = jnp.zeros((NT,), jnp.float32)
    row_pot = jnp.zeros((NS,), jnp.float32)
    for sweep_index in range(ITERS):

        def row_block(rows_in):
            return -row_lse(scores(rows_in) + col_pot[None, :])
        row_pot = lax.map(row_block, blocks).reshape(NS)
        potentials = row_pot.reshape(count, block)

        def col_step(carry, item):
            rows_in, shift = item
            logits = scores(rows_in) + shift[:, None]
            top, total = carry
            higher = jnp.maximum(top, lax.optimization_barrier(jnp.max(logits, axis=0)))
            total = total * jnp.exp(top - higher) + lax.optimization_barrier(jnp.sum(jnp.exp(logits - higher[None, :]), axis=0))
            return ((higher, total), None)
        start = (jnp.full((NT,), -jnp.inf, jnp.float32), jnp.zeros((NT,), jnp.float32))
        (top, total), unused = lax.scan(col_step, start, (blocks, potentials))
        col_pot = -(top + jnp.log(total))
    potentials = row_pot.reshape(count, block)

    def plan_rows(item):
        rows_in, shift = item
        plan = jnp.exp(scores(rows_in) + shift[:, None] + col_pot[None, :]).astype(jnp.bfloat16)
        return jnp.dot(plan, target_words, preferred_element_type=jnp.float32)
    matched = lax.map(plan_rows, (blocks, potentials)).reshape(NS, D)
    source_full = source_words.astype(jnp.float32)
    cov = jnp.dot(source_full.T, matched, precision=highest)
    ortho = cov / jnp.sqrt(jnp.sum(cov * cov) + 1e-06)
    for step_index in range(NEWTON):
        ortho = 1.5 * ortho - 0.5 * jnp.dot(ortho, jnp.dot(ortho.T, ortho, precision=highest), precision=highest)
    rotated = jnp.dot(source_full, ortho, precision=highest).astype(jnp.bfloat16)
    return (rotated, matched, ortho, row_pot, col_pot)
```

```python
import math

import jax
import jax.numpy as jnp
from jax import lax
from jax.experimental import pallas as pl
from jax.experimental.pallas import tpu as pltpu
from jax.sharding import PartitionSpec as P

MESH = pl.DeviceIdType.MESH
F32 = jnp.float32
BF16 = jnp.bfloat16
ITERS = 2
NEWTON = 12
EXACT_STEPS = 3
LN2 = math.log(2.0)
NEG = -1e30
D = 300
DP = 384
DR = 304
NT_OWN = 120


def remote(src, dst, send, recv, device):
    return pltpu.make_async_remote_copy(
        src_ref=src, dst_ref=dst, send_sem=send, recv_sem=recv, device_id=device, device_id_type=MESH
    )


def nt(a, b):
    return lax.dot_general(a, b, (((1,), (1,)), ((), ())), preferred_element_type=F32)


def nn(a, b):
    return jnp.dot(a, b, preferred_element_type=F32)


def split(v):
    hi = v.astype(BF16)
    return hi, (v - hi.astype(F32)).astype(BF16)


def kernel(
    src_ref, tgt_ref, rot_ref, mat_ref, ort_ref, rp_ref, cp_ref,
    s_all, t_all, s_t, logit, rexp, cexp, dense, cmax, csum, rpot, cpot,
    row_out, row_in, col_out, col_in,
    plan, summed, pair_out, pair_in, z_out, z_in,
    cacc, cov_out, cov_pair, rs_out, rs_in, zc_out, zc_in, full, x_ref,
    s_send, s_recv, f_send, t_send, t_recv, row_send, row_recv, col_send, col_recv,
    pair_send, pair_recv, z_send, z_recv, cv_send, cv_recv, rs_send, rs_recv,
    zc_send, zc_recv, ag_send, ag_recv, hf_send, hf_recv,
):
    si = lax.axis_index("src")
    ti = lax.axis_index("tgt")
    x_hi, z = si // 8, si % 8
    x_lo, y, core = ti // 8, (ti // 2) % 4, ti % 2
    other = 1 - core
    g = z * 2 + core
    h = (x_hi * 2 + x_lo) * 4 + y
    partner = (si, x_lo * 8 + y * 2 + other)

    def z_dev(p):
        return (x_hi * 8 + p, ti)

    def s_dev(p):
        return (x_hi * 8 + p // 2, x_lo * 8 + y * 2 + p % 2)

    def t_dev(p):
        return ((p // 8) * 8 + z, ((p // 4) % 2) * 8 + (p % 4) * 2 + core)

    def each(lo, hi, body):
        def step(k, carry):
            body(k)
            return carry
        lax.fori_loop(lo, hi, step, 0)

    s_all[pl.ds(g, 1)] = jnp.zeros((1, 128, DP), BF16)
    t_all[pl.ds(h, 1)] = jnp.zeros((1, 128, DP), BF16)
    s_all[g, :, 0:D] = src_ref[...]
    t_all[h, 0:NT_OWN, 0:D] = tgt_ref[...]

    barrier = pltpu.get_barrier_semaphore()

    def greet(k):
        pl.semaphore_signal(barrier, inc=1, device_id=s_dev((g + k) % 16), device_id_type=MESH)
        pl.semaphore_signal(barrier, inc=1, device_id=t_dev((h + k) % 16), device_id_type=MESH)

    each(1, 16, greet)
    pl.semaphore_wait(barrier, 30)

    def s_copy(k):
        p = (z + k) % 8
        return remote(s_all.at[g], s_all.at[g], s_send.at[k], s_recv.at[g], z_dev(p))

    def s_in(p):
        return remote(s_all.at[p], s_all.at[p], s_send.at[0], s_recv.at[p], partner)

    def forward(p):
        return remote(s_all.at[p], s_all.at[p], f_send.at[p // 2], s_recv.at[p], partner)

    def t_copy(k):
        return remote(t_all.at[h], t_all.at[h], t_send.at[k], t_recv.at[h], t_dev((h + k) % 16))

    def t_in(p):
        return remote(t_all.at[p], t_all.at[p], t_send.at[0], t_recv.at[p], partner)

    forward(g).start()
    each(1, 8, lambda k: s_copy(k).start())
    each(1, 16, lambda k: t_copy(k).start())

    lane = lax.broadcasted_iota(jnp.int32, (8, 128), 1)
    padded = lane >= NT_OWN
    for j in range(16):
        cexp[:, j * 128:(j + 1) * 128] = jnp.where(padded, NEG, 0.0)
    dense[...] = jnp.zeros((128, 128), F32)
    x_ref[...] = jnp.zeros((DP, DP), F32)
    cacc[...] = jnp.zeros((DR, DP), F32)
    cov_out[...] = jnp.zeros(cov_out.shape, F32)

    def relay(k):
        p = ((z + k) % 8) * 2 + core
        s_in(p).wait_recv()
        forward(p).start()

    each(1, 8, relay)
    each(0, 8, lambda k: s_in(k * 2 + other).wait_recv())
    each(1, 16, lambda k: t_in((h + k) % 16).wait_recv())

    scale = 4.0 / math.sqrt(D) / LN2

    def multiply(q):
        piece = t_all[pl.ds(q * 2, 2)].reshape(256, DP)
        at = pl.multiple_of(q * 256, 256)
        for r in range(4):
            rows = s_all[4 * r:4 * r + 4].reshape(512, DP)
            logit[512 * r:512 * r + 512, pl.ds(at, 256)] = nt(rows, piece) * scale

    each(0, 8, multiply)

    def row_pass():
        def block(b):
            for i in range(16):
                v = logit[pl.ds(pl.multiple_of(b * 128 + 8 * i, 8), 8), :] + cexp[...]
                m = jnp.max(v, axis=1, keepdims=True)
                s = jnp.sum(jnp.exp2(v - m), axis=1, keepdims=True)
                lse = m + jnp.log2(s)
                dense[8 * i:8 * i + 8, :] = jnp.where(lane == b, lse, dense[8 * i:8 * i + 8, :])
        each(0, 16, block)

    def col_pass():
        cmax[...] = jnp.full((8, 2048), -3e38, F32)
        csum[...] = jnp.zeros((8, 2048), F32)

        def block(b):
            rows = pl.ds(pl.multiple_of(b * 128, 128), 128)
            for j in range(16):
                cols = slice(j * 128, (j + 1) * 128)
                v = (logit[rows, cols] + rexp[rows, :]).reshape(16, 8, 128)
                old = cmax[:, cols]
                m = jnp.maximum(old, jnp.max(v, axis=0))
                csum[:, cols] = csum[:, cols] * jnp.exp2(old - m) + jnp.sum(jnp.exp2(v - m[None]), axis=0)
                cmax[:, cols] = m
        each(0, 16, block)

    def exchange(out, into, send, recv, me, dev, n):
        each(1, n, lambda k: remote(out, into.at[me], send.at[k], recv.at[me], dev((me + k) % n)).start())
        into[pl.ds(me, 1)] = out[...][None]

        def arrive(k):
            c = remote(out, into.at[(me + k) % n], send.at[k], recv.at[(me + k) % n], dev((me + k) % n))
            c.wait_recv()
            c.wait_send()
        each(1, n, arrive)

    def combined(into):
        a = into[...]
        m = jnp.max(a, axis=0)
        return -(m + jnp.log2(jnp.sum(jnp.exp2(a - m[None]), axis=0)))

    for it in range(ITERS):
        row_pass()
        row_out[it] = dense[...].T[0:16, :]
        exchange(row_out.at[it], row_in.at[it], row_send.at[it], row_recv.at[it], g, s_dev, 16)
        rpot[...] = combined(row_in.at[it])
        dense[0:16, :] = rpot[...]
        turned = dense[...].T
        for b in range(16):
            rexp[b * 128:(b + 1) * 128, :] = jnp.broadcast_to(turned[:, b:b + 1], (128, 128))
        col_pass()
        top = jnp.max(cmax[...], axis=0, keepdims=True)
        whole = jnp.sum(csum[...] * jnp.exp2(cmax[...] - top), axis=0, keepdims=True)
        lse = top + jnp.log2(whole)
        for j in range(16):
            col_out[it, j:j + 1, :] = lse[:, j * 128:(j + 1) * 128]
        exchange(col_out.at[it], col_in.at[it], col_send.at[it], col_recv.at[it], h, t_dev, 16)
        cpot[...] = combined(col_in.at[it])
        for j in range(16):
            cexp[:, j * 128:(j + 1) * 128] = jnp.where(
                padded, NEG, jnp.broadcast_to(cpot[j:j + 1, :], (8, 128))
            )

    rp_ref[...] = rpot[pl.ds(g, 1), :] * LN2
    cp_ref[...] = cpot[pl.ds(h, 1), :] * LN2

    for b in range(16):
        s_t[:, b * 128:(b + 1) * 128] = s_all[b].T

    targets = t_all.reshape(2048, DP)

    def plan_chunk(r):
        def block(b):
            local = pl.ds(pl.multiple_of(b * 128, 128), 128)
            rows = pl.ds(pl.multiple_of(r * 512 + b * 128, 128), 128)
            for j in range(16):
                cols = slice(j * 128, (j + 1) * 128)
                v = logit[rows, cols] + rexp[rows, :] + cexp[0:1, cols]
                plan[local, cols] = jnp.exp2(v).astype(BF16)
        each(0, 4, block)
        piece = nn(plan[...], targets[...])
        summed[pl.ds(r * 4, 4)] = piece.reshape(4, 128, DP)
        hi, lo = split(piece)
        left = s_t[0:DR, pl.ds(pl.multiple_of(r * 512, 512), 512)]
        cacc[...] += nn(left, hi) + nn(left, lo)

    each(0, 4, plan_chunk)

    for half in range(2):
        for l in range(3):
            for r in range(19):
                at = half * 152 + r * 8
                cov_out[half, l * 19 + r] = cacc[at:at + 8, l * 128:(l + 1) * 128]
    cv = remote(cov_out.at[other], cov_pair, cv_send, cv_recv, partner)
    cv.start()

    for p in range(8):
        pair_out[p:p + 1] = summed[pl.ds(2 * p + other, 1)].astype(BF16)
    pr = remote(pair_out, pair_in, pair_send, pair_recv, partner)

    cv.wait()
    pr.start()
    rs_out[...] = (cov_out[pl.ds(core, 1)].reshape(64, 8, 128) + cov_pair[...]).reshape(16, 4, 8, 128)
    each(1, 16, lambda k: remote(
        rs_out.at[(h + k) % 16], rs_in.at[h], rs_send.at[k], rs_recv.at[h], t_dev((h + k) % 16)).start())
    rs_in[pl.ds(h, 1)] = rs_out[pl.ds(h, 1)]

    pr.wait()
    for p in range(8):
        both = summed[pl.ds(2 * p + core, 1)] + pair_in[p:p + 1].astype(F32)
        z_out[p:p + 1] = both.astype(BF16)

    def rs_arrive(k):
        p = (h + k) % 16
        c = remote(rs_out.at[p], rs_in.at[p], rs_send.at[k], rs_recv.at[p], t_dev(p))
        c.wait_recv()
        c.wait_send()
    each(1, 16, rs_arrive)
    zc_out[...] = jnp.sum(rs_in[...], axis=0)
    exchange(zc_out, zc_in, zc_send, zc_recv, z, z_dev, 8)
    mine = jnp.sum(zc_in[...], axis=0)
    full[pl.ds(core, 1), pl.ds(h, 1)] = mine[None, None]

    def ag_copy(k, p):
        return remote(full.at[core, h], full.at[core, h], ag_send.at[k], ag_recv.at[h], t_dev(p))

    each(1, 16, lambda k: ag_copy(k, (h + k) % 16).start())

    def z_copy(k):
        p = (z + k) % 8
        return remote(z_out.at[p], z_in.at[z], z_send.at[k], z_recv.at[z], z_dev(p))
    each(1, 8, lambda k: z_copy(k).start())

    def ag_arrive(k):
        p = (h + k) % 16
        c = remote(full.at[core, p], full.at[core, p], ag_send.at[k], ag_recv.at[p], t_dev(p))
        c.wait_recv()
        c.wait_send()
    each(1, 16, ag_arrive)
    hf = remote(full.at[core], full.at[core], hf_send, hf_recv, partner)
    hf.start()
    hf.wait_send()
    remote(full.at[other], full.at[other], hf_send, hf_recv, partner).wait_recv()

    for half in range(2):
        for l in range(3):
            for r in range(19):
                t = l * 19 + r
                at = half * 152 + r * 8
                x_ref[at:at + 8, l * 128:(l + 1) * 128] = full[half, t // 4, t % 4]

    cov = x_ref[...]
    square = jnp.sum(jnp.sum(cov * cov, axis=0, keepdims=True), axis=1, keepdims=True)
    x_ref[...] = cov / jnp.sqrt(square + 1e-06)
    eye = (
        lax.broadcasted_iota(jnp.int32, (DR, DP), 0) == lax.broadcasted_iota(jnp.int32, (DR, DP), 1)
    ).astype(F32)

    def newton(k):
        v = x_ref[...]
        b = v.astype(BF16)
        rest = (0.5 * (eye - nt(b[0:DR], b))).astype(BF16)
        x_ref[0:DR, :] = v[0:DR] + nn(rest, b)

    def newton_exact(k):
        v = x_ref[...]
        hi, lo = split(v)
        gram = nt(hi[0:DR], hi) + (nt(hi[0:DR], lo) + nt(lo[0:DR], hi))
        rest_hi, rest_lo = split(0.5 * (eye - gram))
        x_ref[0:DR, :] = v[0:DR] + (nn(rest_hi, hi) + (nn(rest_hi, lo) + nn(rest_lo, hi)))

    each(0, NEWTON - EXACT_STEPS, newton)
    each(0, EXACT_STEPS, newton_exact)

    ort_ref[...] = x_ref[0:D, 0:D]
    hi, lo = split(x_ref[...])
    own = s_all[pl.ds(g, 1)].reshape(128, DP)
    rot_ref[...] = (nn(own, hi) + nn(own, lo))[:, 0:D].astype(BF16)

    def z_arrive(k):
        p = (z + k) % 8
        c = remote(z_out.at[p], z_in.at[p], z_send.at[k], z_recv.at[p], z_dev(p))
        c.wait_recv()
        c.wait_send()
    each(1, 8, z_arrive)
    total = summed[pl.ds(g, 1)].reshape(128, DP) + pair_in[pl.ds(z, 1)].reshape(128, DP).astype(F32)
    for k in range(1, 8):
        total = total + z_in[pl.ds((z + k) % 8, 1)].reshape(128, DP).astype(F32)
    mat_ref[...] = total[:, 0:D]

    forward(g).wait_send()
    each(1, 8, lambda k: s_copy(k).wait_send())
    each(1, 8, lambda k: forward(((z + k) % 8) * 2 + core).wait_send())
    each(1, 16, lambda k: t_copy(k).wait_send())


def body(source_words, target_words):
    dma = pltpu.SemaphoreType.DMA
    vmem = pl.BlockSpec(memory_space=pltpu.VMEM)
    rot, mat, ort, rp, cp = pl.pallas_call(
        kernel,
        out_shape=(
            jax.ShapeDtypeStruct((128, D), BF16),
            jax.ShapeDtypeStruct((128, D), F32),
            jax.ShapeDtypeStruct((D, D), F32),
            jax.ShapeDtypeStruct((1, 128), F32),
            jax.ShapeDtypeStruct((1, 128), F32),
        ),
        in_specs=[vmem, vmem],
        out_specs=(vmem,) * 5,
        scratch_shapes=[
            pltpu.VMEM((16, 128, DP), BF16),
            pltpu.VMEM((16, 128, DP), BF16),
            pltpu.VMEM((DP, 2048), BF16),
            pltpu.VMEM((2048, 2048), F32),
            pltpu.VMEM((2048, 128), F32),
            pltpu.VMEM((8, 2048), F32),
            pltpu.VMEM((128, 128), F32),
            pltpu.VMEM((8, 2048), F32),
            pltpu.VMEM((8, 2048), F32),
            pltpu.VMEM((16, 128), F32),
            pltpu.VMEM((16, 128), F32),
            pltpu.VMEM((ITERS, 16, 128), F32),
            pltpu.VMEM((ITERS, 16, 16, 128), F32),
            pltpu.VMEM((ITERS, 16, 128), F32),
            pltpu.VMEM((ITERS, 16, 16, 128), F32),
            pltpu.VMEM((512, 2048), BF16),
            pltpu.VMEM((16, 128, DP), F32),
            pltpu.VMEM((8, 128, DP), BF16),
            pltpu.VMEM((8, 128, DP), BF16),
            pltpu.VMEM((8, 128, DP), BF16),
            pltpu.VMEM((8, 128, DP), BF16),
            pltpu.VMEM((DR, DP), F32),
            pltpu.VMEM((2, 64, 8, 128), F32),
            pltpu.VMEM((64, 8, 128), F32),
            pltpu.VMEM((16, 4, 8, 128), F32),
            pltpu.VMEM((16, 4, 8, 128), F32),
            pltpu.VMEM((4, 8, 128), F32),
            pltpu.VMEM((8, 4, 8, 128), F32),
            pltpu.VMEM((2, 16, 4, 8, 128), F32),
            pltpu.VMEM((DP, DP), F32),
            dma((8,)), dma((16,)), dma((8,)), dma((16,)), dma((16,)),
            dma((ITERS, 16)), dma((ITERS, 16)), dma((ITERS, 16)), dma((ITERS, 16)),
            dma, dma, dma((8,)), dma((8,)), dma, dma, dma((16,)), dma((16,)),
            dma((8,)), dma((8,)), dma((16,)), dma((16,)), dma, dma,
        ],
        compiler_params=pltpu.CompilerParams(
            collective_id=0, has_side_effects=True, vmem_limit_bytes=60 * 1024 * 1024
        ),
    )(source_words, target_words)
    return rot, mat, ort, rp.reshape(128), cp[0, 0:NT_OWN]


def solution(mesh):
    in_specs = (P(("src", "tgt"), None), P(("tgt", "src"), None))
    out_specs = (
        P(("src", "tgt"), None),
        P(("src", "tgt"), None),
        P(),
        P(("src", "tgt")),
        P(("tgt", "src")),
    )
    return jax.shard_map(body, mesh=mesh, in_specs=in_specs, out_specs=out_specs, check_vma=False)
```

```python
import math

import jax
import jax.numpy as jnp
from jax import lax
from jax.experimental import pallas as pl
from jax.experimental.pallas import tpu as pltpu
from jax.sharding import PartitionSpec as P

MESH = pl.DeviceIdType.MESH
F32 = jnp.float32
BF16 = jnp.bfloat16
ITERS = 2
NEWTON = 12
EXACT_STEPS = 2
LN2 = math.log(2.0)
NEG = -1e30
D = 300
DP = 384
DR = 304
NT_OWN = 120
HALVES = ((0, 160), (160, 144))


def remote(src, dst, send, recv, device):
    return pltpu.make_async_remote_copy(
        src_ref=src, dst_ref=dst, send_sem=send, recv_sem=recv, device_id=device, device_id_type=MESH
    )


def nt(a, b):
    return lax.dot_general(a, b, (((1,), (1,)), ((), ())), preferred_element_type=F32)


def nn(a, b):
    return jnp.dot(a, b, preferred_element_type=F32)


def split(v):
    hi = v.astype(BF16)
    return hi, (v - hi.astype(F32)).astype(BF16)


def kernel(
    src_ref, tgt_ref, rot_ref, mat_ref, ort_ref, rp_ref, cp_ref,
    s_all, t_all, t_nat, logit, cexp, rrow, dense, rmax, rsum, lmax, lsum, rpot, cpot,
    row_out, row_in, col_out, col_in,
    plan, summed, pair_out, pair_in, z_out, z_in,
    cacc, cov_out, cov_pair, rs_out, rs_in, zc_out, zc_in, full, x_ref,
    s_send, s_recv, f_send, f_recv, t_send, t_recv, th_recv, row_send, row_recv, col_send, col_recv,
    pair_send, pair_recv, z_send, z_recv, cv_send, cv_recv, rs_send, rs_recv,
    zc_send, zc_recv, ag_send, ag_recv, hf_send, hf_recv,
):
    si = lax.axis_index("src")
    ti = lax.axis_index("tgt")
    x_hi, z = si // 8, si % 8
    x_lo, y, core = ti // 8, (ti // 2) % 4, ti % 2
    other = 1 - core
    g = z * 2 + core
    h = (x_hi * 2 + x_lo) * 4 + y
    partner = (si, x_lo * 8 + y * 2 + other)

    def z_dev(p):
        return (x_hi * 8 + p, ti)

    def s_dev(p):
        return (x_hi * 8 + p // 2, x_lo * 8 + y * 2 + p % 2)

    def t_dev(p):
        return ((p // 8) * 8 + z, ((p // 4) % 2) * 8 + (p % 4) * 2 + core)

    def each(lo, hi, body):
        def step(k, carry):
            body(k)
            return carry
        lax.fori_loop(lo, hi, step, 0)

    s_all[pl.ds(g, 1)] = jnp.zeros((1, DR, 128), BF16)
    t_all[pl.ds(h, 1)] = jnp.zeros((1, DR, 128), BF16)
    s_all[g, 0:D, :] = src_ref[...]
    t_all[h, 0:D, 0:NT_OWN] = tgt_ref[...]

    barrier = pltpu.get_barrier_semaphore()

    def greet(k):
        pl.semaphore_signal(barrier, inc=1, device_id=s_dev((g + k) % 16), device_id_type=MESH)
        pl.semaphore_signal(barrier, inc=1, device_id=t_dev((h + k) % 16), device_id_type=MESH)

    each(1, 16, greet)
    lane = lax.broadcasted_iota(jnp.int32, (8, 128), 1)
    dense[...] = jnp.zeros((128, 128), F32)
    plan[...] = jnp.zeros((2048, 512), BF16)
    x_ref[...] = jnp.zeros((DP, DP), F32)
    cacc[...] = jnp.zeros((DR, DP), F32)
    cov_out[...] = jnp.zeros(cov_out.shape, F32)
    t_nat[pl.ds(h, 1)] = t_all[h].T[None]
    pl.semaphore_wait(barrier, 30)

    def part(slot, half):
        return s_all.at[slot, pl.ds(HALVES[half][0], HALVES[half][1])]

    def s_hop(way, step, half):
        origin = (z + 8 - step) % 8 if way == 0 else (z + step) % 8
        to = (z + 1) % 8 if way == 0 else (z + 7) % 8
        return remote(
            part(origin * 2 + core, half), part(origin * 2 + core, half),
            s_send.at[way, step, half], s_recv.at[origin, half], z_dev(to)
        )

    def s_wait(way, step, half):
        origin = (z + 8 - step) % 8 if way == 0 else (z + step) % 8
        slot = origin * 2 + core
        remote(part(slot, half), part(slot, half), s_send.at[0, 0, 0], s_recv.at[origin, half], partner).wait_recv()

    def hand(p):
        slot = p * 2 + core
        return remote(s_all.at[slot], s_all.at[slot], f_send.at[p], f_recv.at[p], partner)

    def handed(p):
        slot = p * 2 + other
        return remote(s_all.at[slot], s_all.at[slot], f_send.at[0], f_recv.at[p], partner)

    def place(i, j):
        return (x_hi * 2 + x_lo + i * other + j * core) % 4, (y + i * core + j * other) % 4

    def t_slot(i, j):
        px, py = place(i, j)
        return px * 4 + py

    def t_full(i, j, to_i, to_j, n):
        slot = t_slot(i, j)
        return remote(t_all.at[slot], t_all.at[slot], t_send.at[n], t_recv.at[slot], t_dev(t_slot(to_i, to_j)))

    def t_half(i, j, half, to_i, to_j, n):
        slot = t_slot(i, j)
        ref = t_all.at[slot, pl.ds(HALVES[half][0], HALVES[half][1])]
        return remote(ref, ref, t_send.at[n], th_recv.at[slot, half], t_dev(t_slot(to_i, to_j)))

    def t_wait(i, j):
        slot = t_slot(i, j)
        remote(t_all.at[slot], t_all.at[slot], t_send.at[0], t_recv.at[slot], partner).wait_recv()
        t_nat[pl.ds(slot, 1)] = t_all[slot].T[None]

    def t_wait_halves(i, j):
        slot = t_slot(i, j)
        for half in range(2):
            ref = t_all.at[slot, pl.ds(HALVES[half][0], HALVES[half][1])]
            remote(ref, ref, t_send.at[0], th_recv.at[slot, half], partner).wait_recv()
        t_nat[pl.ds(slot, 1)] = t_all[slot].T[None]

    sent = []

    def go(copy):
        copy.start()
        sent.append(copy)

    for half in range(2):
        go(s_hop(0, 0, half))
        go(s_hop(1, 0, half))
    go(t_full(0, 0, 1, 0, 0))
    go(t_full(0, 0, 3, 0, 1))
    go(t_full(0, 0, 0, 1, 2))
    go(t_full(0, 0, 0, 3, 3))
    go(hand(z))

    def s_stage(step):
        for half in range(2):
            for way in range(2):
                s_wait(way, step, half)
                if step < 3 or half == way:
                    go(s_hop(way, step, half))
        go(hand((z + 8 - step) % 8))
        go(hand((z + step) % 8))

    def spread(i, n):
        go(t_full(i, 0, 0, 1, n))
        go(t_full(i, 0, 0, 3, n + 1))

    def spread_halves(i, n):
        t_wait(i, 3)
        go(t_half(i, 3, 0, 0, 1, n))
        t_wait(i, 1)
        go(t_half(i, 1, 1, 0, 3, n + 1))

    t_wait(3, 0)
    go(t_half(3, 0, 0, 1, 0, 4))
    t_wait(1, 0)
    go(t_half(1, 0, 1, 3, 0, 5))
    spread(3, 6)
    spread(1, 8)
    s_stage(1)
    spread_halves(0, 10)
    t_wait_halves(2, 0)
    spread(2, 12)
    s_stage(2)
    spread_halves(3, 14)
    spread_halves(1, 16)
    s_stage(3)
    spread_halves(2, 18)
    far = (z + 4) % 8
    s_wait(0, 4, 0)
    s_wait(1, 4, 1)
    go(hand(far))
    for i in (0, 3, 1, 2):
        t_wait_halves(i, 2)
    each(0, 8, lambda p: handed(p).wait_recv())

    scale = 4.0 / math.sqrt(D) / LN2

    def multiply(q):
        rhs = jnp.concatenate([s_all[2 * q], s_all[2 * q + 1]], axis=1)
        at = pl.ds(pl.multiple_of(q * 256, 256), 256)
        m = jnp.full((8, 256), -3e38, F32)
        total = jnp.zeros((8, 256), F32)
        for r in range(8):
            lhs = t_nat[2 * r:2 * r + 2].reshape(256, DR)
            v = nn(lhs, rhs) * scale
            logit[256 * r:256 * r + 256, at] = v
            v = v.reshape(2, 16, 8, 256)[:, 0:NT_OWN // 8].reshape(NT_OWN // 4, 8, 256)
            old = m
            m = jnp.maximum(old, jnp.max(v, axis=0))
            total = total * jnp.exp2(old - m) + jnp.sum(jnp.exp2(v - m[None]), axis=0)
        rmax[:, at] = m
        rsum[:, at] = total

    each(0, 8, multiply)

    def row_pass():
        rmax[...] = jnp.full((8, 2048), -3e38, F32)
        rsum[...] = jnp.zeros((8, 2048), F32)

        def block(b):
            for j in range(16):
                cols = slice(j * 128, (j + 1) * 128)
                parts = []
                for c in range(2):
                    rows = pl.ds(pl.multiple_of(b * 256 + c * 128, 128), NT_OWN)
                    v = logit[rows, cols] + cexp[rows, :]
                    parts.append(v.reshape(NT_OWN // 8, 8, 128))
                old = rmax[:, cols]
                m = jnp.maximum(jnp.maximum(old, jnp.max(parts[0], axis=0)), jnp.max(parts[1], axis=0))
                rsum[:, cols] = (
                    rsum[:, cols] * jnp.exp2(old - m)
                    + jnp.sum(jnp.exp2(parts[0] - m[None]), axis=0)
                    + jnp.sum(jnp.exp2(parts[1] - m[None]), axis=0)
                )
                rmax[:, cols] = m
        each(0, 8, block)

    def col_pass():
        def block(b):
            for i in range(NT_OWN // 8):
                rows = pl.ds(pl.multiple_of(b * 128 + 8 * i, 8), 8)
                v = [
                    logit[rows, j * 128:(j + 1) * 128] + rrow[:, j * 128:(j + 1) * 128]
                    for j in range(16)
                ]
                m = v[0]
                for w in v[1:]:
                    m = jnp.maximum(m, w)
                total = jnp.exp2(v[0] - m)
                for w in v[1:]:
                    total = total + jnp.exp2(w - m)
                lmax[rows, :] = m
                lsum[rows, :] = total
        each(0, 16, block)
        for i in range(NT_OWN // 8):
            column = jnp.zeros((8, 128), F32)
            for b in range(16):
                rows = slice(b * 128 + 8 * i, b * 128 + 8 * i + 8)
                m = lmax[rows, :]
                top = jnp.max(m, axis=1, keepdims=True)
                whole = jnp.sum(lsum[rows, :] * jnp.exp2(m - top), axis=1, keepdims=True)
                column = jnp.where(lane == b, top + jnp.log2(whole), column)
            dense[8 * i:8 * i + 8, :] = column

    def exchange(out, into, send, recv, me, dev, n):
        each(1, n, lambda k: remote(out, into.at[me], send.at[k], recv.at[me], dev((me + k) % n)).start())
        into[pl.ds(me, 1)] = out[...][None]

        def arrive(k):
            c = remote(out, into.at[(me + k) % n], send.at[k], recv.at[(me + k) % n], dev((me + k) % n))
            c.wait_recv()
            c.wait_send()
        each(1, n, arrive)

    def combined(into):
        a = into[...]
        m = jnp.max(a, axis=0)
        return -(m + jnp.log2(jnp.sum(jnp.exp2(a - m[None]), axis=0)))

    for it in range(ITERS):
        if it:
            row_pass()
        top = jnp.max(rmax[...], axis=0, keepdims=True)
        whole = jnp.sum(rsum[...] * jnp.exp2(rmax[...] - top), axis=0, keepdims=True)
        lse = top + jnp.log2(whole)
        for j in range(16):
            row_out[it, j:j + 1, :] = lse[:, j * 128:(j + 1) * 128]
        exchange(row_out.at[it], row_in.at[it], row_send.at[it], row_recv.at[it], g, s_dev, 16)
        rpot[...] = combined(row_in.at[it])
        for j in range(16):
            rrow[:, j * 128:(j + 1) * 128] = jnp.broadcast_to(rpot[j:j + 1, :], (8, 128))
        col_pass()
        col_out[it] = dense[...].T[0:16, :]
        exchange(col_out.at[it], col_in.at[it], col_send.at[it], col_recv.at[it], h, t_dev, 16)
        cpot[...] = combined(col_in.at[it])
        dense[0:16, :] = cpot[...]
        turned = dense[...].T
        for b in range(16):
            cexp[b * 128:(b + 1) * 128, :] = jnp.broadcast_to(turned[:, b:b + 1], (128, 128))

    rp_ref[...] = (rpot[pl.ds(g, 1), :] * LN2).reshape(128)
    cp_ref[...] = (cpot[pl.ds(h, 1), :] * LN2)[:, 0:NT_OWN].reshape(NT_OWN)

    def plan_chunk(r):
        def block(b):
            rows = pl.ds(pl.multiple_of(b * 128, 128), NT_OWN)
            for j in range(4):
                cols = pl.ds(pl.multiple_of(r * 512 + j * 128, 128), 128)
                v = logit[rows, cols] + cexp[rows, :] + rrow[0:1, cols]
                plan[rows, j * 128:(j + 1) * 128] = jnp.exp2(v).astype(BF16)
        each(0, 16, block)
        targets = jnp.concatenate([t_all[b] for b in range(16)], axis=1)
        piece = nn(targets, plan[...])
        for j in range(4):
            summed[pl.ds(r * 4 + j, 1)] = piece[:, j * 128:(j + 1) * 128][None]
        hi, lo = split(piece)
        left = jnp.concatenate([s_all[r * 4 + j] for j in range(4)], axis=1)
        cacc[:, 0:DR] += nt(left, hi) + nt(left, lo)

    each(0, 4, plan_chunk)

    for half in range(2):
        for l in range(3):
            for r in range(19):
                at = half * 152 + r * 8
                cov_out[half, l * 19 + r] = cacc[at:at + 8, l * 128:(l + 1) * 128]
    cv = remote(cov_out.at[other], cov_pair, cv_send, cv_recv, partner)
    cv.start()

    for p in range(8):
        pair_out[p:p + 1] = summed[pl.ds(2 * p + other, 1)].astype(BF16)
    pr = remote(pair_out, pair_in, pair_send, pair_recv, partner)

    cv.wait()
    pr.start()
    rs_out[...] = (cov_out[pl.ds(core, 1)].reshape(64, 8, 128) + cov_pair[...]).reshape(16, 4, 8, 128)
    each(1, 16, lambda k: remote(
        rs_out.at[(h + k) % 16], rs_in.at[h], rs_send.at[k], rs_recv.at[h], t_dev((h + k) % 16)).start())
    rs_in[pl.ds(h, 1)] = rs_out[pl.ds(h, 1)]

    pr.wait()
    for p in range(8):
        both = summed[pl.ds(2 * p + core, 1)] + pair_in[p:p + 1].astype(F32)
        z_out[p:p + 1] = both.astype(BF16)

    def rs_arrive(k):
        p = (h + k) % 16
        c = remote(rs_out.at[p], rs_in.at[p], rs_send.at[k], rs_recv.at[p], t_dev(p))
        c.wait_recv()
        c.wait_send()
    each(1, 16, rs_arrive)
    zc_out[...] = jnp.sum(rs_in[...], axis=0)
    exchange(zc_out, zc_in, zc_send, zc_recv, z, z_dev, 8)
    mine = jnp.sum(zc_in[...], axis=0)
    full[pl.ds(core, 1), pl.ds(h, 1)] = mine[None, None]

    def ag_copy(k, p):
        return remote(full.at[core, h], full.at[core, h], ag_send.at[k], ag_recv.at[h], t_dev(p))

    each(1, 16, lambda k: ag_copy(k, (h + k) % 16).start())

    def z_copy(k):
        p = (z + k) % 8
        return remote(z_out.at[p], z_in.at[z], z_send.at[k], z_recv.at[z], z_dev(p))
    each(1, 8, lambda k: z_copy(k).start())

    def ag_arrive(k):
        p = (h + k) % 16
        c = remote(full.at[core, p], full.at[core, p], ag_send.at[k], ag_recv.at[p], t_dev(p))
        c.wait_recv()
        c.wait_send()
    each(1, 16, ag_arrive)
    hf = remote(full.at[core], full.at[core], hf_send, hf_recv, partner)
    hf.start()
    hf.wait_send()
    remote(full.at[other], full.at[other], hf_send, hf_recv, partner).wait_recv()

    for half in range(2):
        for l in range(3):
            for r in range(19):
                t = l * 19 + r
                at = half * 152 + r * 8
                x_ref[at:at + 8, l * 128:(l + 1) * 128] = full[half, t // 4, t % 4]

    cov = x_ref[...]
    square = jnp.sum(jnp.sum(cov * cov, axis=0, keepdims=True), axis=1, keepdims=True)
    x_ref[...] = cov / jnp.sqrt(square + 1e-06)
    eye = (
        lax.broadcasted_iota(jnp.int32, (DR, DP), 0) == lax.broadcasted_iota(jnp.int32, (DR, DP), 1)
    ).astype(F32)

    def newton(k):
        v = x_ref[...]
        b = v.astype(BF16)
        rest = (0.5 * (eye - nt(b[0:DR], b))).astype(BF16)
        x_ref[0:DR, :] = v[0:DR] + nn(rest, b)

    def newton_exact(k):
        v = x_ref[...]
        hi, lo = split(v)
        gram = nt(hi[0:DR], hi) + (nt(hi[0:DR], lo) + nt(lo[0:DR], hi))
        rest_hi, rest_lo = split(0.5 * (eye - gram))
        x_ref[0:DR, :] = v[0:DR] + (nn(rest_hi, hi) + (nn(rest_hi, lo) + nn(rest_lo, hi)))

    each(0, NEWTON - EXACT_STEPS, newton)
    each(0, EXACT_STEPS, newton_exact)

    ort_ref[...] = x_ref[0:D, 0:D]
    hi, lo = split(x_ref[...].T[0:DR, 0:DR])
    own = s_all[pl.ds(g, 1)].reshape(DR, 128)
    rot_ref[...] = (nn(hi, own) + nn(lo, own))[0:D, :].astype(BF16)

    def z_arrive(k):
        p = (z + k) % 8
        c = remote(z_out.at[p], z_in.at[p], z_send.at[k], z_recv.at[p], z_dev(p))
        c.wait_recv()
        c.wait_send()
    each(1, 8, z_arrive)
    total = summed[pl.ds(g, 1)].reshape(DR, 128) + pair_in[pl.ds(z, 1)].reshape(DR, 128).astype(F32)
    for k in range(1, 8):
        total = total + z_in[pl.ds((z + k) % 8, 1)].reshape(DR, 128).astype(F32)
    mat_ref[...] = total[0:D, :]

    for copy in sent:
        copy.wait_send()


def body(source_words, target_words):
    dma = pltpu.SemaphoreType.DMA
    vmem = pl.BlockSpec(memory_space=pltpu.VMEM)
    rot, mat, ort, rp, cp = pl.pallas_call(
        kernel,
        out_shape=(
            jax.ShapeDtypeStruct((D, 128), BF16),
            jax.ShapeDtypeStruct((D, 128), F32),
            jax.ShapeDtypeStruct((D, D), F32),
            jax.ShapeDtypeStruct((128,), F32),
            jax.ShapeDtypeStruct((NT_OWN,), F32),
        ),
        in_specs=[vmem, vmem],
        out_specs=(vmem,) * 5,
        scratch_shapes=[
            pltpu.VMEM((16, DR, 128), BF16),
            pltpu.VMEM((16, DR, 128), BF16),
            pltpu.VMEM((16, 128, DR), BF16),
            pltpu.VMEM((2048, 2048), F32),
            pltpu.VMEM((2048, 128), F32),
            pltpu.VMEM((8, 2048), F32),
            pltpu.VMEM((128, 128), F32),
            pltpu.VMEM((8, 2048), F32),
            pltpu.VMEM((8, 2048), F32),
            pltpu.VMEM((2048, 128), F32),
            pltpu.VMEM((2048, 128), F32),
            pltpu.VMEM((16, 128), F32),
            pltpu.VMEM((16, 128), F32),
            pltpu.VMEM((ITERS, 16, 128), F32),
            pltpu.VMEM((ITERS, 16, 16, 128), F32),
            pltpu.VMEM((ITERS, 16, 128), F32),
            pltpu.VMEM((ITERS, 16, 16, 128), F32),
            pltpu.VMEM((2048, 512), BF16),
            pltpu.VMEM((16, DR, 128), F32),
            pltpu.VMEM((8, DR, 128), BF16),
            pltpu.VMEM((8, DR, 128), BF16),
            pltpu.VMEM((8, DR, 128), BF16),
            pltpu.VMEM((8, DR, 128), BF16),
            pltpu.VMEM((DR, DP), F32),
            pltpu.VMEM((2, 64, 8, 128), F32),
            pltpu.VMEM((64, 8, 128), F32),
            pltpu.VMEM((16, 4, 8, 128), F32),
            pltpu.VMEM((16, 4, 8, 128), F32),
            pltpu.VMEM((4, 8, 128), F32),
            pltpu.VMEM((8, 4, 8, 128), F32),
            pltpu.VMEM((2, 16, 4, 8, 128), F32),
            pltpu.VMEM((DP, DP), F32),
            dma((2, 4, 2)), dma((8, 2)), dma((8,)), dma((8,)), dma((22,)), dma((16,)), dma((16, 2)),
            dma((ITERS, 16)), dma((ITERS, 16)), dma((ITERS, 16)), dma((ITERS, 16)),
            dma, dma, dma((8,)), dma((8,)), dma, dma, dma((16,)), dma((16,)),
            dma((8,)), dma((8,)), dma((16,)), dma((16,)), dma, dma,
        ],
        compiler_params=pltpu.CompilerParams(
            collective_id=0, has_side_effects=True, vmem_limit_bytes=60 * 1024 * 1024
        ),
    )(source_words.T, target_words.T)
    return rot.T, mat.T, ort, rp, cp


def solution(mesh):
    in_specs = (P(("src", "tgt"), None), P(("tgt", "src"), None))
    out_specs = (
        P(("src", "tgt"), None),
        P(("src", "tgt"), None),
        P(),
        P(("src", "tgt")),
        P(("tgt", "src")),
    )
    return jax.shard_map(body, mesh=mesh, in_specs=in_specs, out_specs=out_specs, check_vma=False)
```

```python
import math

import jax
import jax.numpy as jnp
from jax import lax
from jax.experimental import pallas as pl
from jax.experimental.pallas import tpu as pltpu
from jax.sharding import PartitionSpec as P

MESH = pl.DeviceIdType.MESH
F32 = jnp.float32
BF16 = jnp.bfloat16
ITERS = 2
NEWTON = 12
EXACT_STEPS = 2
LN2 = math.log(2.0)
NEG = -1e30
D = 300
DP = 384
DR = 304
NT_OWN = 120
HALVES = ((0, 160), (160, 144))


def remote(src, dst, send, recv, device):
    return pltpu.make_async_remote_copy(
        src_ref=src, dst_ref=dst, send_sem=send, recv_sem=recv, device_id=device, device_id_type=MESH
    )


def nt(a, b):
    return lax.dot_general(a, b, (((1,), (1,)), ((), ())), preferred_element_type=F32)


def nn(a, b):
    return jnp.dot(a, b, preferred_element_type=F32)


def split(v):
    hi = v.astype(BF16)
    return hi, (v - hi.astype(F32)).astype(BF16)


def kernel(
    src_ref, tgt_ref, rot_ref, mat_ref, ort_ref, rp_ref, cp_ref,
    s_all, t_all, t_nat, logit, cexp, rrow, dense, rmax, rsum, lmax, lsum, rpot, cpot,
    row_out, row_in, col_out, col_in,
    plan, lines, summed, pair_in, z_out, z_in,
    cacc, cov_out, cov_pair, rs_out, rs_in, zc_out, zc_in, full, x_ref,
    s_send, s_recv, f_send, f_recv, t_send, t_recv, th_recv, row_send, row_recv, col_send, col_recv,
    pair_send, pair_recv, z_send, z_recv, cv_send, cv_recv, rs_send, rs_recv,
    zc_send, zc_recv, ag_send, ag_recv, hf_send, hf_recv,
):
    si = lax.axis_index("src")
    ti = lax.axis_index("tgt")
    x_hi, z = si // 8, si % 8
    x_lo, y, core = ti // 8, (ti // 2) % 4, ti % 2
    other = 1 - core
    g = z * 2 + core
    h = (x_hi * 2 + x_lo) * 4 + y
    partner = (si, x_lo * 8 + y * 2 + other)

    def z_dev(p):
        return (x_hi * 8 + p, ti)

    def s_dev(p):
        return (x_hi * 8 + p // 2, x_lo * 8 + y * 2 + p % 2)

    def t_dev(p):
        return ((p // 8) * 8 + z, ((p // 4) % 2) * 8 + (p % 4) * 2 + core)

    def each(lo, hi, body):
        def step(k, carry):
            body(k)
            return carry
        lax.fori_loop(lo, hi, step, 0)

    s_all[0] = jnp.zeros((DR, 128), BF16)
    t_all[0] = jnp.zeros((DR, 128), BF16)
    s_all[0, 0:D, :] = src_ref[...]
    t_all[0, 0:D, 0:NT_OWN] = tgt_ref[...]

    def place(i, j):
        return (x_hi * 2 + x_lo + i * other + j * core) % 4, (y + i * core + j * other) % 4

    def t_slot(i, j):
        px, py = place(i, j)
        return px * 4 + py

    barrier = pltpu.get_barrier_semaphore()
    near = [partner, z_dev((z + 1) % 8), z_dev((z + 7) % 8)]
    near += [t_dev(t_slot(*at)) for at in ((1, 0), (3, 0), (2, 0), (0, 1), (0, 3))]
    for device in near:
        pl.semaphore_signal(barrier, inc=1, device_id=device, device_id_type=MESH)
    lane = lax.broadcasted_iota(jnp.int32, (8, 128), 1)
    dense[...] = jnp.zeros((128, 128), F32)
    for b in range(16):
        plan[b * 128 + NT_OWN:(b + 1) * 128, :] = jnp.zeros((128 - NT_OWN, 2048), BF16)
    x_ref[...] = jnp.zeros((DP, DP), F32)
    cacc[...] = jnp.zeros((DR, DP), F32)
    cov_out[...] = jnp.zeros(cov_out.shape, F32)
    t_nat[0] = t_all[0].T
    rmax[...] = jnp.full((8, 2048), -3e38, F32)
    rsum[...] = jnp.zeros((8, 2048), F32)
    pl.semaphore_wait(barrier, 8)

    def part(slot, half):
        return s_all.at[slot, pl.ds(HALVES[half][0], HALVES[half][1])]

    def s_hop(way, step, half):
        here = (8 - step) % 8 if way == 0 else step
        there = (here + 7) % 8 if way == 0 else here + 1
        to = (z + 1) % 8 if way == 0 else (z + 7) % 8
        return remote(
            part(2 * here, half), part(2 * there, half),
            s_send.at[way, step, half], s_recv.at[there, half], z_dev(to)
        )

    def s_wait(way, step, half):
        k = (8 - step) % 8 if way == 0 else step
        remote(part(2 * k, half), part(2 * k, half), s_send.at[0, 0, 0], s_recv.at[k, half], partner).wait_recv()

    def hand(k):
        return remote(s_all.at[2 * k], s_all.at[2 * k + 1], f_send.at[k], f_recv.at[k], partner)

    def handed(k):
        return remote(s_all.at[2 * k], s_all.at[2 * k + 1], f_send.at[0], f_recv.at[k], partner)

    def moved(i, j, to_i, to_j):
        return ((i - to_i) % 4) * 4 + (j - to_j) % 4

    def t_full(i, j, to_i, to_j, n):
        there = moved(i, j, to_i, to_j)
        return remote(
            t_all.at[4 * i + j], t_all.at[there], t_send.at[n], t_recv.at[there], t_dev(t_slot(to_i, to_j))
        )

    def t_half(i, j, half, to_i, to_j, n):
        there = moved(i, j, to_i, to_j)
        rows = pl.ds(HALVES[half][0], HALVES[half][1])
        return remote(
            t_all.at[4 * i + j, rows], t_all.at[there, rows],
            t_send.at[n], th_recv.at[there, half], t_dev(t_slot(to_i, to_j))
        )

    def t_wait(i, j):
        slot = 4 * i + j
        remote(t_all.at[slot], t_all.at[slot], t_send.at[0], t_recv.at[slot], partner).wait_recv()
        t_nat[slot] = t_all[slot].T

    def t_wait_halves(i, j):
        slot = 4 * i + j
        for half in range(2):
            ref = t_all.at[slot, pl.ds(HALVES[half][0], HALVES[half][1])]
            remote(ref, ref, t_send.at[0], th_recv.at[slot, half], partner).wait_recv()
        t_nat[slot] = t_all[slot].T

    sent = []

    def go(copy):
        copy.start()
        sent.append(copy)

    for half in range(2):
        go(s_hop(0, 0, half))
        go(s_hop(1, 0, half))
    go(t_full(0, 0, 1, 0, 0))
    go(t_full(0, 0, 3, 0, 1))
    go(t_full(0, 0, 0, 1, 2))
    go(t_full(0, 0, 0, 3, 3))
    go(t_full(0, 0, 2, 0, 4))
    go(hand(0))

    def s_stage(step):
        for half in range(2):
            for way in range(2):
                s_wait(way, step, half)
                if step < 3 or half == way:
                    go(s_hop(way, step, half))
        go(hand(8 - step))
        go(hand(step))

    def spread(i, n):
        go(t_full(i, 0, 0, 1, n))
        go(t_full(i, 0, 0, 3, n + 1))

    def spread_halves(i, n):
        t_wait(i, 3)
        go(t_half(i, 3, 0, 0, 1, n))
        t_wait(i, 1)
        go(t_half(i, 1, 1, 0, 3, n + 1))

    scale = 4.0 / math.sqrt(D) / LN2

    def tile(p, places):
        rhs = jnp.concatenate([s_all[2 * p], s_all[2 * p + 1]], axis=1)
        at = pl.ds(pl.multiple_of(p * 256, 256), 256)
        slots = [4 * i + j for i, j in places]
        m = rmax[:, at]
        total = rsum[:, at]
        for n in range(0, len(slots), 2):
            pair = slots[n:n + 2]
            v = nn(jnp.concatenate([t_nat[slot] for slot in pair], axis=0), rhs) * scale
            parts = []
            for k, slot in enumerate(pair):
                w = v[k * 128:k * 128 + 128]
                logit[slot * 128:slot * 128 + 128, at] = w
                parts.append(w[0:NT_OWN].reshape(NT_OWN // 8, 8, 256))
            w = jnp.concatenate(parts, axis=0)
            old = m
            m = jnp.maximum(old, jnp.max(w, axis=0))
            total = total * jnp.exp2(old - m) + jnp.sum(jnp.exp2(w - m[None]), axis=0)
        rmax[:, at] = m
        rsum[:, at] = total

    def tiles(first, n, places):
        for k in range(n):
            tile((first + k) % 8, places)

    first_five = ((0, 0), (1, 0), (3, 0), (0, 1), (0, 3))
    t_wait(3, 0)
    t_wait(1, 0)
    spread(3, 6)
    spread(1, 8)
    s_stage(1)
    t_wait(2, 0)
    spread(2, 12)
    spread_halves(0, 10)
    for k in (0, 1, 7):
        handed(k).wait_recv()
    tiles(7, 3, first_five)
    s_stage(2)
    spread_halves(3, 14)
    spread_halves(1, 16)
    for k in (2, 6):
        handed(k).wait_recv()
        tile(k, first_five)
    s_stage(3)
    spread_halves(2, 18)
    ring = ((2, 0), (3, 3), (3, 1), (1, 3), (1, 1), (2, 3), (2, 1))
    tiles(6, 5, ring[0:4])
    s_wait(0, 4, 0)
    s_wait(1, 4, 1)
    go(hand(4))
    tiles(6, 5, ring[4:])
    for k in (3, 5, 4):
        handed(k).wait_recv()
        tile(k, first_five)
    tiles(3, 3, ring)
    for i in (0, 3, 1, 2):
        t_wait_halves(i, 2)
    tiles(0, 8, ((0, 2), (1, 2), (2, 2), (3, 2)))

    def row_again():
        rsum[...] = jnp.zeros((8, 2048), F32)

        def block(b):
            rows = pl.ds(pl.multiple_of(b * 128, 128), NT_OWN)
            for j in range(16):
                cols = slice(j * 128, (j + 1) * 128)
                v = jnp.exp2(logit[rows, cols] + cexp[rows, :] + rrow[0:1, cols])
                logit[rows, cols] = v
                rsum[:, cols] += jnp.sum(v.reshape(NT_OWN // 8, 8, 128), axis=0)
        each(0, 16, block)

    def col_again():
        def block(b):
            rows = pl.ds(pl.multiple_of(b * 128, 128), NT_OWN)
            total = jnp.zeros((NT_OWN, 128), F32)
            for j in range(16):
                cols = slice(j * 128, (j + 1) * 128)
                total = total + logit[rows, cols] * rrow[0:1, cols]
            lsum[rows, :] = total
        each(0, 16, block)
        for i in range(NT_OWN // 8):
            column = jnp.zeros((8, 128), F32)
            for b in range(16):
                rows = slice(b * 128 + 8 * i, b * 128 + 8 * i + 8)
                column = jnp.where(lane == b, jnp.sum(lsum[rows, :], axis=1, keepdims=True), column)
            dense[8 * i:8 * i + 8, :] = column

    def col_pass():
        def block(b):
            for i in range(NT_OWN // 8):
                rows = pl.ds(pl.multiple_of(b * 128 + 8 * i, 8), 8)
                v = [
                    logit[rows, j * 128:(j + 1) * 128] + rrow[:, j * 128:(j + 1) * 128]
                    for j in range(16)
                ]
                m = v[0]
                for w in v[1:]:
                    m = jnp.maximum(m, w)
                total = jnp.exp2(v[0] - m)
                for w in v[1:]:
                    total = total + jnp.exp2(w - m)
                lmax[rows, :] = m
                lsum[rows, :] = total
        each(0, 16, block)
        for i in range(NT_OWN // 8):
            column = jnp.zeros((8, 128), F32)
            for b in range(16):
                rows = slice(b * 128 + 8 * i, b * 128 + 8 * i + 8)
                m = lmax[rows, :]
                top = jnp.max(m, axis=1, keepdims=True)
                whole = jnp.sum(lsum[rows, :] * jnp.exp2(m - top), axis=1, keepdims=True)
                column = jnp.where(lane == b, top + jnp.log2(whole), column)
            dense[8 * i:8 * i + 8, :] = column

    def exchange(out, into, send, recv, me, dev, n):
        each(1, n, lambda k: remote(out, into.at[me], send.at[k], recv.at[me], dev((me + k) % n)).start())
        into[pl.ds(me, 1)] = out[...][None]

        def arrive(k):
            c = remote(out, into.at[(me + k) % n], send.at[k], recv.at[(me + k) % n], dev((me + k) % n))
            c.wait_recv()
            c.wait_send()
        each(1, n, arrive)

    def combined(into):
        a = into[...]
        m = jnp.max(a, axis=0)
        return -(m + jnp.log2(jnp.sum(jnp.exp2(a - m[None]), axis=0)))

    def s_order(r):
        return ((z + r // 2) % 8) * 2 + (core if r % 2 == 0 else other)

    def t_order(r):
        return t_slot(r // 4, r % 4)

    def to_rows(ref):
        for r in range(16):
            rrow[:, r * 128:(r + 1) * 128] = jnp.broadcast_to(ref[pl.ds(s_order(r), 1), :], (8, 128))

    def out_row(it, values):
        for r in range(16):
            row_out[it, pl.ds(s_order(r), 1), :] = values[:, r * 128:(r + 1) * 128]

    def out_col(it):
        lines[...] = dense[...].T[0:16, :]
        for r in range(16):
            col_out[it, pl.ds(t_order(r), 1), :] = lines[r:r + 1, :]

    def to_cols(ref):
        for r in range(16):
            dense[r:r + 1, :] = ref[pl.ds(t_order(r), 1), :]
        turned = dense[...].T
        for b in range(16):
            cexp[b * 128:(b + 1) * 128, :] = jnp.broadcast_to(turned[:, b:b + 1], (128, 128))

    top = jnp.max(rmax[...], axis=0, keepdims=True)
    whole = jnp.sum(rsum[...] * jnp.exp2(rmax[...] - top), axis=0, keepdims=True)
    out_row(0, top + jnp.log2(whole))
    exchange(row_out.at[0], row_in.at[0], row_send.at[0], row_recv.at[0], g, s_dev, 16)
    rpot[...] = combined(row_in.at[0])
    to_rows(rpot)
    col_pass()
    out_col(0)
    exchange(col_out.at[0], col_in.at[0], col_send.at[0], col_recv.at[0], h, t_dev, 16)
    cpot[...] = combined(col_in.at[0])
    to_cols(cpot)

    row_again()
    out_row(1, jnp.sum(rsum[...], axis=0, keepdims=True))
    exchange(row_out.at[1], row_in.at[1], row_send.at[1], row_recv.at[1], g, s_dev, 16)
    whole = jnp.sum(row_in[1], axis=0)
    rpot[...] = rpot[...] - jnp.log2(whole)
    lines[...] = 1.0 / whole
    to_rows(lines)
    col_again()
    out_col(1)
    exchange(col_out.at[1], col_in.at[1], col_send.at[1], col_recv.at[1], h, t_dev, 16)
    whole = jnp.sum(col_in[1], axis=0)
    cpot[...] = cpot[...] - jnp.log2(whole)
    lines[...] = 1.0 / whole
    to_cols(lines)

    rp_ref[...] = (rpot[pl.ds(g, 1), :] * LN2).reshape(128)
    cp_ref[...] = (cpot[pl.ds(h, 1), :] * LN2)[:, 0:NT_OWN].reshape(NT_OWN)

    def fill(q):
        for b in range(16):
            rows = slice(b * 128, b * 128 + NT_OWN)
            share = cexp[rows, :]
            for j in range(4):
                cols = slice(q * 512 + j * 128, q * 512 + j * 128 + 128)
                plan[rows, cols] = (logit[rows, cols] * rrow[0:1, cols] * share).astype(BF16)

    targets = jnp.concatenate([t_all[b] for b in range(16)], axis=1)
    fill(0)
    for q in range(4):
        if q < 3:
            fill(q + 1)
        piece = nn(targets, plan[:, q * 512:(q + 1) * 512])
        for j in range(4):
            summed[4 * q + j] = piece[:, j * 128:(j + 1) * 128]
        cacc[:, 0:DR] += nt(piece.astype(BF16), jnp.concatenate([s_all[4 * q + j] for j in range(4)], axis=1))

    for half in range(2):
        at = half * 152
        for r in range(19):
            for l in range(2):
                cov_out[half, l * 19 + r] = cacc[at + 8 * r:at + 8 * r + 8, l * 128:(l + 1) * 128]
        for r in range(10):
            last = cacc[at + 8 * r:at + 8 * r + 8, 256:384]
            if r < 9:
                last = last + pltpu.roll(cacc[at + 80 + 8 * r:at + 88 + 8 * r, 256:384], 64, 1)
            cov_out[half, 38 + r] = last
    cv = remote(cov_out.at[other], cov_pair, cv_send, cv_recv, partner)
    cv.start()

    pr = [
        remote(summed.at[2 * k + 1], pair_in.at[k], pair_send.at[k], pair_recv.at[k], partner) for k in range(8)
    ]

    cv.wait()
    for copy in pr:
        copy.start()
    rs_out[...] = (cov_out[pl.ds(core, 1)].reshape(48, 8, 128) + cov_pair[...]).reshape(16, 24, 128).astype(BF16)
    each(1, 16, lambda k: remote(
        rs_out.at[(h + k) % 16], rs_in.at[h], rs_send.at[k], rs_recv.at[h], t_dev((h + k) % 16)).start())
    rs_in[pl.ds(h, 1)] = rs_out[pl.ds(h, 1)]

    for k in range(1, 8):
        pr[k].wait_recv()
        z_out[k] = (summed[2 * k] + pair_in[k]).astype(BF16)

    def rs_arrive(k):
        p = (h + k) % 16
        c = remote(rs_out.at[p], rs_in.at[p], rs_send.at[k], rs_recv.at[p], t_dev(p))
        c.wait_recv()
        c.wait_send()
    each(1, 16, rs_arrive)
    zc_out[...] = jnp.sum(rs_in[...].astype(F32), axis=0).reshape(3, 8, 128)
    exchange(zc_out, zc_in, zc_send, zc_recv, z, z_dev, 8)
    mine = jnp.sum(zc_in[...], axis=0)
    full[pl.ds(core, 1), pl.ds(h, 1)] = mine[None, None]

    def ag_copy(k, p):
        return remote(full.at[core, h], full.at[core, h], ag_send.at[k], ag_recv.at[h], t_dev(p))

    each(1, 16, lambda k: ag_copy(k, (h + k) % 16).start())

    def z_copy(k):
        return remote(z_out.at[k], z_in.at[k], z_send.at[k], z_recv.at[k], z_dev((z + k) % 8))
    each(1, 8, lambda k: z_copy(k).start())

    def ag_arrive(k):
        p = (h + k) % 16
        c = remote(full.at[core, p], full.at[core, p], ag_send.at[k], ag_recv.at[p], t_dev(p))
        c.wait_recv()
        c.wait_send()
    each(1, 16, ag_arrive)
    hf = remote(full.at[core], full.at[core], hf_send, hf_recv, partner)
    hf.start()
    hf.wait_send()
    remote(full.at[other], full.at[other], hf_send, hf_recv, partner).wait_recv()

    def tile_of(half, t):
        return full[half, t // 3, t % 3]

    for half in range(2):
        at = half * 152
        for r in range(19):
            for l in range(2):
                x_ref[at + 8 * r:at + 8 * r + 8, l * 128:(l + 1) * 128] = tile_of(half, l * 19 + r)
        for r in range(10):
            last = tile_of(half, 38 + r)
            x_ref[at + 8 * r:at + 8 * r + 8, 256:384] = jnp.where(lane < 44, last, 0.0)
            if r < 9:
                x_ref[at + 80 + 8 * r:at + 88 + 8 * r, 256:384] = jnp.where(lane < 44, pltpu.roll(last, 64, 1), 0.0)

    cov = x_ref[...]
    square = jnp.sum(jnp.sum(cov * cov, axis=0, keepdims=True), axis=1, keepdims=True)
    x_ref[...] = cov / jnp.sqrt(square + 1e-06)
    eye = (
        lax.broadcasted_iota(jnp.int32, (DR, DP), 0) == lax.broadcasted_iota(jnp.int32, (DR, DP), 1)
    ).astype(F32)

    def newton(k):
        v = x_ref[...]
        b = v.astype(BF16)
        rest = (0.5 * (eye - nt(b[0:DR], b))).astype(BF16)
        x_ref[0:DR, :] = v[0:DR] + nn(rest, b)

    def newton_exact(k):
        v = x_ref[...]
        hi, lo = split(v)
        gram = nt(hi[0:DR], hi) + (nt(hi[0:DR], lo) + nt(lo[0:DR], hi))
        rest_hi, rest_lo = split(0.5 * (eye - gram))
        x_ref[0:DR, :] = v[0:DR] + (nn(rest_hi, hi) + (nn(rest_hi, lo) + nn(rest_lo, hi)))

    each(0, NEWTON - EXACT_STEPS, newton)
    each(0, EXACT_STEPS, newton_exact)

    ort_ref[...] = x_ref[...].T[0:D, 0:D]
    hi, lo = split(x_ref[0:DR, 0:DR])
    own = s_all[0]
    rot_ref[...] = (nn(hi, own) + nn(lo, own))[0:D, :].astype(BF16)

    each(1, 8, lambda k: z_copy(k).wait())
    pr[0].wait_recv()
    total = summed[0] + pair_in[0]
    for k in range(1, 8):
        total = total + z_in[k].astype(F32)
    mat_ref[...] = total[0:D, :]

    for copy in sent + pr:
        copy.wait_send()


def store(*refs):
    for given, result in zip(refs[:5], refs[5:]):
        result[...] = given[...]


def body(source_words, target_words):
    dma = pltpu.SemaphoreType.DMA
    vmem = pl.BlockSpec(memory_space=pltpu.VMEM)
    results = pl.pallas_call(
        kernel,
        out_shape=(
            jax.ShapeDtypeStruct((D, 128), BF16),
            jax.ShapeDtypeStruct((D, 128), F32),
            jax.ShapeDtypeStruct((D, D), F32),
            jax.ShapeDtypeStruct((128,), F32),
            jax.ShapeDtypeStruct((NT_OWN,), F32),
        ),
        in_specs=[vmem, vmem],
        out_specs=(vmem,) * 5,
        scratch_shapes=[
            pltpu.VMEM((16, DR, 128), BF16),
            pltpu.VMEM((16, DR, 128), BF16),
            pltpu.VMEM((16, 128, DR), BF16),
            pltpu.VMEM((2048, 2048), F32),
            pltpu.VMEM((2048, 128), F32),
            pltpu.VMEM((8, 2048), F32),
            pltpu.VMEM((128, 128), F32),
            pltpu.VMEM((8, 2048), F32),
            pltpu.VMEM((8, 2048), F32),
            pltpu.VMEM((2048, 128), F32),
            pltpu.VMEM((2048, 128), F32),
            pltpu.VMEM((16, 128), F32),
            pltpu.VMEM((16, 128), F32),
            pltpu.VMEM((ITERS, 16, 128), F32),
            pltpu.VMEM((ITERS, 16, 16, 128), F32),
            pltpu.VMEM((ITERS, 16, 128), F32),
            pltpu.VMEM((ITERS, 16, 16, 128), F32),
            pltpu.VMEM((2048, 2048), BF16),
            pltpu.VMEM((16, 128), F32),
            pltpu.VMEM((16, DR, 128), F32),
            pltpu.VMEM((8, DR, 128), F32),
            pltpu.VMEM((8, DR, 128), BF16),
            pltpu.VMEM((8, DR, 128), BF16),
            pltpu.VMEM((DR, DP), F32),
            pltpu.VMEM((2, 48, 8, 128), F32),
            pltpu.VMEM((48, 8, 128), F32),
            pltpu.VMEM((16, 24, 128), BF16),
            pltpu.VMEM((16, 24, 128), BF16),
            pltpu.VMEM((3, 8, 128), F32),
            pltpu.VMEM((8, 3, 8, 128), F32),
            pltpu.VMEM((2, 16, 3, 8, 128), F32),
            pltpu.VMEM((DP, DP), F32),
            dma((2, 4, 2)), dma((8, 2)), dma((8,)), dma((8,)), dma((22,)), dma((16,)), dma((16, 2)),
            dma((ITERS, 16)), dma((ITERS, 16)), dma((ITERS, 16)), dma((ITERS, 16)),
            dma((8,)), dma((8,)), dma((8,)), dma((8,)), dma, dma, dma((16,)), dma((16,)),
            dma((8,)), dma((8,)), dma((16,)), dma((16,)), dma, dma,
        ],
        compiler_params=pltpu.CompilerParams(
            collective_id=0, has_side_effects=True, vmem_limit_bytes=60 * 1024 * 1024
        ),
    )(source_words.T, target_words.T)
    rot, mat, ort, rp, cp = pl.pallas_call(
        store,
        out_shape=tuple(jax.ShapeDtypeStruct(r.shape, r.dtype) for r in results),
        in_specs=[vmem] * 5,
        out_specs=(vmem,) * 5,
    )(*results)
    return rot.T, mat.T, ort, rp, cp


def solution(mesh):
    in_specs = (P(("src", "tgt"), None), P(("tgt", "src"), None))
    out_specs = (
        P(("src", "tgt"), None),
        P(("src", "tgt"), None),
        P(),
        P(("src", "tgt")),
        P(("tgt", "src")),
    )
    return jax.shard_map(body, mesh=mesh, in_specs=in_specs, out_specs=out_specs, check_vma=False)
```

```python
import math

import jax
import jax.numpy as jnp
from jax import lax
from jax.experimental import pallas as pl
from jax.experimental.pallas import tpu as pltpu
from jax.sharding import PartitionSpec as P

MESH = pl.DeviceIdType.MESH
F32 = jnp.float32
BF16 = jnp.bfloat16
ITERS = 2
NEWTON = 12
SMALL_STEPS = 5
EXACT_STEPS = 1
LN2 = math.log(2.0)
NEG = -1e30
D = 300
DP = 384
DR = 304
NT_OWN = 120
HALVES = ((0, 160), (160, 144))


def remote(src, dst, send, recv, device):
    return pltpu.make_async_remote_copy(
        src_ref=src, dst_ref=dst, send_sem=send, recv_sem=recv, device_id=device, device_id_type=MESH
    )


def nt(a, b):
    return lax.dot_general(a, b, (((1,), (1,)), ((), ())), preferred_element_type=F32)


def nn(a, b):
    return jnp.dot(a, b, preferred_element_type=F32)


def split(v):
    hi = v.astype(BF16)
    return hi, (v - hi.astype(F32)).astype(BF16)


def kernel(
    src_ref, tgt_ref, rot_ref, mat_ref, ort_ref, rp_ref, cp_ref,
    s_all, t_all, t_nat, logit, cexp, rrow, dense, rmax, rsum, lmax, lsum, rpot, cpot,
    row_out, row_in, col_out, col_in,
    plan, lines, summed, pair_in, z_out, z_in,
    cacc, cov_out, cov_pair, rs_out, rs_in, zc_out, zc_in, full, x_ref,
    s_send, s_recv, f_send, f_recv, t_send, t_recv, th_recv, row_send, row_recv, col_send, col_recv,
    pair_send, pair_recv, z_send, z_recv, cv_send, cv_recv, rs_send, rs_recv,
    zc_send, zc_recv, ag_send, ag_recv, hf_send, hf_recv,
):
    si = lax.axis_index("src")
    ti = lax.axis_index("tgt")
    x_hi, z = si // 8, si % 8
    x_lo, y, core = ti // 8, (ti // 2) % 4, ti % 2
    other = 1 - core
    g = z * 2 + core
    h = (x_hi * 2 + x_lo) * 4 + y
    partner = (si, x_lo * 8 + y * 2 + other)

    def z_dev(p):
        return (x_hi * 8 + p, ti)

    def s_dev(p):
        return (x_hi * 8 + p // 2, x_lo * 8 + y * 2 + p % 2)

    def t_dev(p):
        return ((p // 8) * 8 + z, ((p // 4) % 2) * 8 + (p % 4) * 2 + core)

    def each(lo, hi, body):
        def step(k, carry):
            body(k)
            return carry
        lax.fori_loop(lo, hi, step, 0)

    s_all[0] = jnp.zeros((DR, 128), BF16)
    t_all[0] = jnp.zeros((DR, 128), BF16)
    s_all[0, 0:D, :] = src_ref[...]
    t_all[0, 0:D, 0:NT_OWN] = tgt_ref[...]

    def place(i, j):
        return (x_hi * 2 + x_lo + i * other + j * core) % 4, (y + i * core + j * other) % 4

    def t_slot(i, j):
        px, py = place(i, j)
        return px * 4 + py

    barrier = pltpu.get_barrier_semaphore()
    near = [partner, z_dev((z + 1) % 8), z_dev((z + 7) % 8)]
    near += [t_dev(t_slot(*at)) for at in ((1, 0), (3, 0), (2, 0), (0, 1), (0, 3))]
    for device in near:
        pl.semaphore_signal(barrier, inc=1, device_id=device, device_id_type=MESH)
    lane = lax.broadcasted_iota(jnp.int32, (8, 128), 1)
    dense[...] = jnp.zeros((128, 128), F32)
    for b in range(16):
        plan[b * 128 + NT_OWN:(b + 1) * 128, :] = jnp.zeros((128 - NT_OWN, 2048), BF16)
    x_ref[...] = jnp.zeros((DP, DP), F32)
    cacc[...] = jnp.zeros((DR, DP), F32)
    cov_out[...] = jnp.zeros(cov_out.shape, F32)
    t_nat[0] = t_all[0].T
    rmax[...] = jnp.full((8, 2048), -3e38, F32)
    rsum[...] = jnp.zeros((8, 2048), F32)
    pl.semaphore_wait(barrier, 8)

    def part(slot, half):
        return s_all.at[slot, pl.ds(HALVES[half][0], HALVES[half][1])]

    def s_hop(way, step, half):
        here = (8 - step) % 8 if way == 0 else step
        there = (here + 7) % 8 if way == 0 else here + 1
        to = (z + 1) % 8 if way == 0 else (z + 7) % 8
        return remote(
            part(2 * here, half), part(2 * there, half),
            s_send.at[way, step, half], s_recv.at[there, half], z_dev(to)
        )

    def s_wait(way, step, half):
        k = (8 - step) % 8 if way == 0 else step
        remote(part(2 * k, half), part(2 * k, half), s_send.at[0, 0, 0], s_recv.at[k, half], partner).wait_recv()

    def hand(k):
        return remote(s_all.at[2 * k], s_all.at[2 * k + 1], f_send.at[k], f_recv.at[k], partner)

    def handed(k):
        return remote(s_all.at[2 * k], s_all.at[2 * k + 1], f_send.at[0], f_recv.at[k], partner)

    def moved(i, j, to_i, to_j):
        return ((i - to_i) % 4) * 4 + (j - to_j) % 4

    def t_full(i, j, to_i, to_j, n):
        there = moved(i, j, to_i, to_j)
        return remote(
            t_all.at[4 * i + j], t_all.at[there], t_send.at[n], t_recv.at[there], t_dev(t_slot(to_i, to_j))
        )

    def t_half(i, j, half, to_i, to_j, n):
        there = moved(i, j, to_i, to_j)
        rows = pl.ds(HALVES[half][0], HALVES[half][1])
        return remote(
            t_all.at[4 * i + j, rows], t_all.at[there, rows],
            t_send.at[n], th_recv.at[there, half], t_dev(t_slot(to_i, to_j))
        )

    def t_wait(i, j):
        slot = 4 * i + j
        remote(t_all.at[slot], t_all.at[slot], t_send.at[0], t_recv.at[slot], partner).wait_recv()
        t_nat[slot] = t_all[slot].T

    def t_wait_halves(i, j):
        slot = 4 * i + j
        for half in range(2):
            ref = t_all.at[slot, pl.ds(HALVES[half][0], HALVES[half][1])]
            remote(ref, ref, t_send.at[0], th_recv.at[slot, half], partner).wait_recv()
        t_nat[slot] = t_all[slot].T

    sent = []

    def go(copy):
        copy.start()
        sent.append(copy)

    for half in range(2):
        go(s_hop(0, 0, half))
        go(s_hop(1, 0, half))
    go(t_full(0, 0, 1, 0, 0))
    go(t_full(0, 0, 3, 0, 1))
    go(t_full(0, 0, 0, 1, 2))
    go(t_full(0, 0, 0, 3, 3))
    go(t_full(0, 0, 2, 0, 4))
    go(hand(0))

    def s_stage(step):
        for half in range(2):
            for way in range(2):
                s_wait(way, step, half)
                if step < 3 or half == way:
                    go(s_hop(way, step, half))
        go(hand(8 - step))
        go(hand(step))

    def spread(i, n):
        go(t_full(i, 0, 0, 1, n))
        go(t_full(i, 0, 0, 3, n + 1))

    def spread_halves(i, n):
        t_wait(i, 3)
        go(t_half(i, 3, 0, 0, 1, n))
        t_wait(i, 1)
        go(t_half(i, 1, 1, 0, 3, n + 1))

    scale = 4.0 / math.sqrt(D) / LN2

    def tile(p, places):
        rhs = jnp.concatenate([s_all[2 * p], s_all[2 * p + 1]], axis=1)
        at = pl.ds(pl.multiple_of(p * 256, 256), 256)
        slots = [4 * i + j for i, j in places]
        m = rmax[:, at]
        total = rsum[:, at]
        for n in range(0, len(slots), 2):
            pair = slots[n:n + 2]
            v = nn(jnp.concatenate([t_nat[slot] for slot in pair], axis=0), rhs) * scale
            parts = []
            for k, slot in enumerate(pair):
                w = v[k * 128:k * 128 + 128]
                logit[slot * 128:slot * 128 + 128, at] = w
                parts.append(w[0:NT_OWN].reshape(NT_OWN // 8, 8, 256))
            w = jnp.concatenate(parts, axis=0)
            old = m
            m = jnp.maximum(old, jnp.max(w, axis=0))
            total = total * jnp.exp2(old - m) + jnp.sum(jnp.exp2(w - m[None]), axis=0)
        rmax[:, at] = m
        rsum[:, at] = total

    def tiles(first, n, places):
        for k in range(n):
            tile((first + k) % 8, places)

    first_five = ((0, 0), (1, 0), (3, 0), (0, 1), (0, 3))
    t_wait(3, 0)
    t_wait(1, 0)
    spread(3, 6)
    spread(1, 8)
    s_stage(1)
    t_wait(2, 0)
    spread(2, 12)
    spread_halves(0, 10)
    for k in (0, 1, 7):
        handed(k).wait_recv()
    tiles(7, 3, first_five)
    s_stage(2)
    spread_halves(3, 14)
    spread_halves(1, 16)
    for k in (2, 6):
        handed(k).wait_recv()
        tile(k, first_five)
    s_stage(3)
    spread_halves(2, 18)
    ring = ((2, 0), (3, 3), (3, 1), (1, 3), (1, 1), (2, 3), (2, 1))
    tiles(6, 5, ring)
    for k in (3, 5):
        handed(k).wait_recv()
        tile(k, first_five)
    s_wait(0, 4, 0)
    s_wait(1, 4, 1)
    go(hand(4))
    tile(3, ring)
    tile(5, ring)
    handed(4).wait_recv()
    tile(4, first_five + ring)
    for i in (0, 3, 1, 2):
        t_wait_halves(i, 2)
    tiles(0, 8, ((0, 2), (1, 2), (2, 2), (3, 2)))

    def row_again():
        rsum[...] = jnp.zeros((8, 2048), F32)

        def block(b):
            rows = pl.ds(pl.multiple_of(b * 128, 128), NT_OWN)
            for j in range(16):
                cols = slice(j * 128, (j + 1) * 128)
                v = jnp.exp2(logit[rows, cols] + cexp[rows, :] + rrow[0:1, cols])
                logit[rows, cols] = v
                rsum[:, cols] += jnp.sum(v.reshape(NT_OWN // 8, 8, 128), axis=0)
        each(0, 16, block)

    def col_again():
        def block(b):
            rows = pl.ds(pl.multiple_of(b * 128, 128), NT_OWN)
            total = jnp.zeros((NT_OWN, 128), F32)
            for j in range(16):
                cols = slice(j * 128, (j + 1) * 128)
                total = total + logit[rows, cols] * rrow[0:1, cols]
            lsum[rows, :] = total
        each(0, 16, block)
        for i in range(NT_OWN // 8):
            column = jnp.zeros((8, 128), F32)
            for b in range(16):
                rows = slice(b * 128 + 8 * i, b * 128 + 8 * i + 8)
                column = jnp.where(lane == b, jnp.sum(lsum[rows, :], axis=1, keepdims=True), column)
            dense[8 * i:8 * i + 8, :] = column

    def col_pass():
        def block(b):
            for i in range(NT_OWN // 8):
                rows = pl.ds(pl.multiple_of(b * 128 + 8 * i, 8), 8)
                v = [
                    logit[rows, j * 128:(j + 1) * 128] + rrow[:, j * 128:(j + 1) * 128]
                    for j in range(16)
                ]
                m = v[0]
                for w in v[1:]:
                    m = jnp.maximum(m, w)
                total = jnp.exp2(v[0] - m)
                for w in v[1:]:
                    total = total + jnp.exp2(w - m)
                lmax[rows, :] = m
                lsum[rows, :] = total
        each(0, 16, block)
        for i in range(NT_OWN // 8):
            column = jnp.zeros((8, 128), F32)
            for b in range(16):
                rows = slice(b * 128 + 8 * i, b * 128 + 8 * i + 8)
                m = lmax[rows, :]
                top = jnp.max(m, axis=1, keepdims=True)
                whole = jnp.sum(lsum[rows, :] * jnp.exp2(m - top), axis=1, keepdims=True)
                column = jnp.where(lane == b, top + jnp.log2(whole), column)
            dense[8 * i:8 * i + 8, :] = column

    z_peers = [((z + k) % 8, z_dev((z + k) % 8)) for k in (4, 3, 5, 2, 6, 1, 7)]
    s_peers = []
    for k in (4, 3, 5, 2, 6, 1, 7, 0):
        for c in range(2):
            if k or c:
                slot = ((z + k) % 8) * 2 + (other if c else core)
                s_peers.append((slot, s_dev(slot)))
    t_peers = []
    for d in sorted(range(1, 16), key=lambda d: -(min(d // 4, 4 - d // 4) + min(d % 4, 4 - d % 4))):
        px, py = (x_hi * 2 + x_lo + d // 4) % 4, (y + d % 4) % 4
        t_peers.append((px * 4 + py, ((px // 2) * 8 + z, (px % 2) * 8 + py * 2 + core)))

    def exchange(out, into, send, recv, me, peers):
        for n, (slot, device) in enumerate(peers):
            remote(out, into.at[me], send.at[n], recv.at[me], device).start()
        into[pl.ds(me, 1)] = out[...][None]
        for n, (slot, device) in reversed(list(enumerate(peers))):
            copy = remote(out, into.at[slot], send.at[n], recv.at[slot], device)
            copy.wait_recv()
            copy.wait_send()

    def combined(into):
        a = into[...]
        m = jnp.max(a, axis=0)
        return -(m + jnp.log2(jnp.sum(jnp.exp2(a - m[None]), axis=0)))

    def s_order(r):
        return ((z + r // 2) % 8) * 2 + (core if r % 2 == 0 else other)

    def t_order(r):
        return t_slot(r // 4, r % 4)

    def to_rows(ref):
        for r in range(16):
            rrow[:, r * 128:(r + 1) * 128] = jnp.broadcast_to(ref[pl.ds(s_order(r), 1), :], (8, 128))

    def out_row(it, values):
        for r in range(16):
            row_out[it, pl.ds(s_order(r), 1), :] = values[:, r * 128:(r + 1) * 128]

    def out_col(it):
        lines[...] = dense[...].T[0:16, :]
        for r in range(16):
            col_out[it, pl.ds(t_order(r), 1), :] = lines[r:r + 1, :]

    def to_cols(ref):
        for r in range(16):
            dense[r:r + 1, :] = ref[pl.ds(t_order(r), 1), :]
        turned = dense[...].T
        for b in range(16):
            cexp[b * 128:(b + 1) * 128, :] = jnp.broadcast_to(turned[:, b:b + 1], (128, 128))

    top = jnp.max(rmax[...], axis=0, keepdims=True)
    whole = jnp.sum(rsum[...] * jnp.exp2(rmax[...] - top), axis=0, keepdims=True)
    out_row(0, top + jnp.log2(whole))
    exchange(row_out.at[0], row_in.at[0], row_send.at[0], row_recv.at[0], g, s_peers)
    rpot[...] = combined(row_in.at[0])
    to_rows(rpot)
    col_pass()
    out_col(0)
    exchange(col_out.at[0], col_in.at[0], col_send.at[0], col_recv.at[0], h, t_peers)
    cpot[...] = combined(col_in.at[0])
    to_cols(cpot)

    row_again()
    out_row(1, jnp.sum(rsum[...], axis=0, keepdims=True))
    exchange(row_out.at[1], row_in.at[1], row_send.at[1], row_recv.at[1], g, s_peers)
    whole = jnp.sum(row_in[1], axis=0)
    rpot[...] = rpot[...] - jnp.log2(whole)
    lines[...] = 1.0 / whole
    to_rows(lines)
    col_again()
    out_col(1)
    exchange(col_out.at[1], col_in.at[1], col_send.at[1], col_recv.at[1], h, t_peers)
    whole = jnp.sum(col_in[1], axis=0)
    cpot[...] = cpot[...] - jnp.log2(whole)
    lines[...] = 1.0 / whole
    to_cols(lines)

    rp_ref[...] = (rpot[pl.ds(g, 1), :] * LN2).reshape(128)
    cp_ref[...] = (cpot[pl.ds(h, 1), :] * LN2)[:, 0:NT_OWN].reshape(NT_OWN)

    def fill(q):
        for b in range(16):
            rows = slice(b * 128, b * 128 + NT_OWN)
            share = cexp[rows, :]
            for j in range(4):
                cols = slice(q * 512 + j * 128, q * 512 + j * 128 + 128)
                plan[rows, cols] = (logit[rows, cols] * rrow[0:1, cols] * share).astype(BF16)

    targets = jnp.concatenate([t_all[b] for b in range(16)], axis=1)
    fill(0)
    for q in range(4):
        if q < 3:
            fill(q + 1)
        piece = nn(targets, plan[:, q * 512:(q + 1) * 512])
        for j in range(4):
            summed[4 * q + j] = piece[:, j * 128:(j + 1) * 128]
        cacc[:, 0:DR] += nt(piece.astype(BF16), jnp.concatenate([s_all[4 * q + j] for j in range(4)], axis=1))

    for half in range(2):
        at = half * 152
        for r in range(19):
            for l in range(2):
                cov_out[half, l * 19 + r] = cacc[at + 8 * r:at + 8 * r + 8, l * 128:(l + 1) * 128]
        for r in range(10):
            last = cacc[at + 8 * r:at + 8 * r + 8, 256:384]
            if r < 9:
                last = last + pltpu.roll(cacc[at + 80 + 8 * r:at + 88 + 8 * r, 256:384], 64, 1)
            cov_out[half, 38 + r] = last
    cv = remote(cov_out.at[other], cov_pair, cv_send, cv_recv, partner)
    cv.start()

    pr = [
        remote(summed.at[2 * k + 1], pair_in.at[k], pair_send.at[k], pair_recv.at[k], partner) for k in range(8)
    ]

    cv.wait()
    for copy in pr:
        copy.start()
    rs_out[...] = (cov_out[pl.ds(core, 1)].reshape(48, 8, 128) + cov_pair[...]).reshape(16, 24, 128).astype(BF16)
    for n, (slot, device) in enumerate(t_peers):
        remote(rs_out.at[slot], rs_in.at[h], rs_send.at[n], rs_recv.at[h], device).start()
    rs_in[pl.ds(h, 1)] = rs_out[pl.ds(h, 1)]

    for k in range(1, 8):
        pr[k].wait_recv()
        z_out[k] = (summed[2 * k] + pair_in[k]).astype(BF16)

    for n, (slot, device) in reversed(list(enumerate(t_peers))):
        copy = remote(rs_out.at[slot], rs_in.at[slot], rs_send.at[n], rs_recv.at[slot], device)
        copy.wait_recv()
        copy.wait_send()
    zc_out[...] = jnp.sum(rs_in[...].astype(F32), axis=0).reshape(3, 8, 128)
    exchange(zc_out, zc_in, zc_send, zc_recv, z, z_peers)
    mine = jnp.sum(zc_in[...], axis=0)
    full[pl.ds(core, 1), pl.ds(h, 1)] = mine[None, None]

    for n, (slot, device) in enumerate(t_peers):
        remote(full.at[core, h], full.at[core, h], ag_send.at[n], ag_recv.at[h], device).start()

    def pass_on(slot):
        return remote(full.at[core, slot], full.at[core, slot], hf_send.at[slot], hf_recv.at[slot], partner)

    pass_on(h).start()

    def z_copy(k):
        return remote(z_out.at[k], z_in.at[k], z_send.at[k], z_recv.at[k], z_dev((z + k) % 8))
    each(1, 8, lambda k: z_copy(k).start())

    for n, (slot, device) in reversed(list(enumerate(t_peers))):
        copy = remote(full.at[core, slot], full.at[core, slot], ag_send.at[n], ag_recv.at[slot], device)
        copy.wait_recv()
        pass_on(slot).start()
        copy.wait_send()
    for slot in range(16):
        remote(full.at[other, slot], full.at[other, slot], hf_send.at[slot], hf_recv.at[slot], partner).wait_recv()

    def tile_of(half, t):
        return full[half, t // 3, t % 3]

    for half in range(2):
        at = half * 152
        for r in range(19):
            for l in range(2):
                x_ref[at + 8 * r:at + 8 * r + 8, l * 128:(l + 1) * 128] = tile_of(half, l * 19 + r)
        for r in range(10):
            last = tile_of(half, 38 + r)
            x_ref[at + 8 * r:at + 8 * r + 8, 256:384] = jnp.where(lane < 44, last, 0.0)
            if r < 9:
                x_ref[at + 80 + 8 * r:at + 88 + 8 * r, 256:384] = jnp.where(lane < 44, pltpu.roll(last, 64, 1), 0.0)

    cov = x_ref[...]
    square = jnp.sum(jnp.sum(cov * cov, axis=0, keepdims=True), axis=1, keepdims=True)
    x_ref[...] = cov / jnp.sqrt(square + 1e-06)
    eye = (
        lax.broadcasted_iota(jnp.int32, (DR, DP), 0) == lax.broadcasted_iota(jnp.int32, (DR, DP), 1)
    ).astype(F32)

    def newton_small(k):
        v = x_ref[0:DR, :]
        b = x_ref[...].astype(BF16)
        gram = nt(b[0:DR], b).astype(BF16)
        x_ref[0:DR, :] = 1.5 * v - 0.5 * nn(gram, b)

    def newton(k):
        v = x_ref[...]
        b = v.astype(BF16)
        rest = (0.5 * (eye - nt(b[0:DR], b))).astype(BF16)
        x_ref[0:DR, :] = v[0:DR] + nn(rest, b)

    def newton_exact(k):
        v = x_ref[...]
        hi, lo = split(v)
        gram = nt(hi[0:DR], hi) + (nt(hi[0:DR], lo) + nt(lo[0:DR], hi))
        rest_hi, rest_lo = split(0.5 * (eye - gram))
        x_ref[0:DR, :] = v[0:DR] + (nn(rest_hi, hi) + (nn(rest_hi, lo) + nn(rest_lo, hi)))

    each(0, SMALL_STEPS, newton_small)
    each(SMALL_STEPS, NEWTON - EXACT_STEPS, newton)
    each(0, EXACT_STEPS, newton_exact)

    ort_ref[...] = x_ref[...].T[0:D, 0:D]
    hi, lo = split(x_ref[0:DR, 0:DR])
    own = s_all[0]
    rot_ref[...] = (nn(hi, own) + nn(lo, own))[0:D, :].astype(BF16)

    each(1, 8, lambda k: z_copy(k).wait())
    pr[0].wait_recv()
    total = summed[0] + pair_in[0]
    for k in range(1, 8):
        total = total + z_in[k].astype(F32)
    mat_ref[...] = total[0:D, :]

    for copy in sent + pr:
        copy.wait_send()
    for slot in range(16):
        pass_on(slot).wait_send()


def store(*refs):
    for given, result in zip(refs[:5], refs[5:]):
        result[...] = given[...]


def body(source_words, target_words):
    dma = pltpu.SemaphoreType.DMA
    vmem = pl.BlockSpec(memory_space=pltpu.VMEM)
    results = pl.pallas_call(
        kernel,
        out_shape=(
            jax.ShapeDtypeStruct((D, 128), BF16),
            jax.ShapeDtypeStruct((D, 128), F32),
            jax.ShapeDtypeStruct((D, D), F32),
            jax.ShapeDtypeStruct((128,), F32),
            jax.ShapeDtypeStruct((NT_OWN,), F32),
        ),
        in_specs=[vmem, vmem],
        out_specs=(vmem,) * 5,
        scratch_shapes=[
            pltpu.VMEM((16, DR, 128), BF16),
            pltpu.VMEM((16, DR, 128), BF16),
            pltpu.VMEM((16, 128, DR), BF16),
            pltpu.VMEM((2048, 2048), F32),
            pltpu.VMEM((2048, 128), F32),
            pltpu.VMEM((8, 2048), F32),
            pltpu.VMEM((128, 128), F32),
            pltpu.VMEM((8, 2048), F32),
            pltpu.VMEM((8, 2048), F32),
            pltpu.VMEM((2048, 128), F32),
            pltpu.VMEM((2048, 128), F32),
            pltpu.VMEM((16, 128), F32),
            pltpu.VMEM((16, 128), F32),
            pltpu.VMEM((ITERS, 16, 128), F32),
            pltpu.VMEM((ITERS, 16, 16, 128), F32),
            pltpu.VMEM((ITERS, 16, 128), F32),
            pltpu.VMEM((ITERS, 16, 16, 128), F32),
            pltpu.VMEM((2048, 2048), BF16),
            pltpu.VMEM((16, 128), F32),
            pltpu.VMEM((16, DR, 128), F32),
            pltpu.VMEM((8, DR, 128), F32),
            pltpu.VMEM((8, DR, 128), BF16),
            pltpu.VMEM((8, DR, 128), BF16),
            pltpu.VMEM((DR, DP), F32),
            pltpu.VMEM((2, 48, 8, 128), F32),
            pltpu.VMEM((48, 8, 128), F32),
            pltpu.VMEM((16, 24, 128), BF16),
            pltpu.VMEM((16, 24, 128), BF16),
            pltpu.VMEM((3, 8, 128), F32),
            pltpu.VMEM((8, 3, 8, 128), F32),
            pltpu.VMEM((2, 16, 3, 8, 128), F32),
            pltpu.VMEM((DP, DP), F32),
            dma((2, 4, 2)), dma((8, 2)), dma((8,)), dma((8,)), dma((22,)), dma((16,)), dma((16, 2)),
            dma((ITERS, 16)), dma((ITERS, 16)), dma((ITERS, 16)), dma((ITERS, 16)),
            dma((8,)), dma((8,)), dma((8,)), dma((8,)), dma, dma, dma((16,)), dma((16,)),
            dma((8,)), dma((8,)), dma((16,)), dma((16,)), dma((16,)), dma((16,)),
        ],
        compiler_params=pltpu.CompilerParams(
            collective_id=0, has_side_effects=True, vmem_limit_bytes=60 * 1024 * 1024
        ),
    )(source_words.T, target_words.T)
    rot, mat, ort, rp, cp = pl.pallas_call(
        store,
        out_shape=tuple(jax.ShapeDtypeStruct(r.shape, r.dtype) for r in results),
        in_specs=[vmem] * 5,
        out_specs=(vmem,) * 5,
    )(*results)
    return rot.T, mat.T, ort, rp, cp


def solution(mesh):
    in_specs = (P(("src", "tgt"), None), P(("tgt", "src"), None))
    out_specs = (
        P(("src", "tgt"), None),
        P(("src", "tgt"), None),
        P(),
        P(("src", "tgt")),
        P(("tgt", "src")),
    )
    return jax.shard_map(body, mesh=mesh, in_specs=in_specs, out_specs=out_specs, check_vma=False)
```

```python
import math

import jax
import jax.numpy as jnp
from jax import lax
from jax.experimental import pallas as pl
from jax.experimental.pallas import tpu as pltpu
from jax.sharding import PartitionSpec as P

MESH = pl.DeviceIdType.MESH
F32 = jnp.float32
BF16 = jnp.bfloat16
ITERS = 2
NEWTON = 12
SMALL_STEPS = 5
EXACT_STEPS = 1
LN2 = math.log(2.0)
NEG = -1e30
D = 300
DP = 384
DR = 304
NT_OWN = 120
HALVES = ((0, 160), (160, 144))


def remote(src, dst, send, recv, device):
    return pltpu.make_async_remote_copy(
        src_ref=src, dst_ref=dst, send_sem=send, recv_sem=recv, device_id=device, device_id_type=MESH
    )


def nt(a, b):
    return lax.dot_general(a, b, (((1,), (1,)), ((), ())), preferred_element_type=F32)


def nn(a, b):
    return jnp.dot(a, b, preferred_element_type=F32)


def split(v):
    hi = v.astype(BF16)
    return hi, (v - hi.astype(F32)).astype(BF16)


def kernel(
    src_ref, tgt_ref, rot_ref, mat_ref, ort_ref, rp_ref, cp_ref,
    s_all, t_all, t_nat, logit, cexp, rrow, dense, rmax, rsum, lmax, lsum, rpot, cpot,
    row_out, row_in, col_out, col_in,
    plan, lines, summed, pair_in, z_out, z_in,
    cacc, cov_out, cov_pair, rs_out, rs_in, zc_out, zc_in, full, x_ref,
    s_send, s_recv, f_send, f_recv, t_send, t_recv, th_recv, row_send, row_recv, col_send, col_recv,
    pair_send, pair_recv, z_send, z_recv, cv_send, cv_recv, rs_send, rs_recv,
    zc_send, zc_recv, ag_send, ag_recv, hf_send, hf_recv,
):
    si = lax.axis_index("src")
    ti = lax.axis_index("tgt")
    x_hi, z = si // 8, si % 8
    x_lo, y, core = ti // 8, (ti // 2) % 4, ti % 2
    other = 1 - core
    g = z * 2 + core
    h = (x_hi * 2 + x_lo) * 4 + y
    partner = (si, x_lo * 8 + y * 2 + other)

    def z_dev(p):
        return (x_hi * 8 + p, ti)

    def s_dev(p):
        return (x_hi * 8 + p // 2, x_lo * 8 + y * 2 + p % 2)

    def t_dev(p):
        return ((p // 8) * 8 + z, ((p // 4) % 2) * 8 + (p % 4) * 2 + core)

    def each(lo, hi, body):
        def step(k, carry):
            body(k)
            return carry
        lax.fori_loop(lo, hi, step, 0)

    s_all[0] = jnp.zeros((DR, 128), BF16)
    t_all[0] = jnp.zeros((DR, 128), BF16)
    s_all[0, 0:D, :] = src_ref[...]
    t_all[0, 0:D, 0:NT_OWN] = tgt_ref[...]

    def place(i, j):
        return (x_hi * 2 + x_lo + i * other + j * core) % 4, (y + i * core + j * other) % 4

    def t_slot(i, j):
        px, py = place(i, j)
        return px * 4 + py

    barrier = pltpu.get_barrier_semaphore()
    near = [partner, z_dev((z + 1) % 8), z_dev((z + 7) % 8)]
    near += [t_dev(t_slot(*at)) for at in ((1, 0), (3, 0), (2, 0), (0, 1), (0, 3))]
    for device in near:
        pl.semaphore_signal(barrier, inc=1, device_id=device, device_id_type=MESH)
    lane = lax.broadcasted_iota(jnp.int32, (8, 128), 1)
    dense[...] = jnp.zeros((128, 128), F32)
    for b in range(16):
        plan[b * 128 + NT_OWN:(b + 1) * 128, :] = jnp.zeros((128 - NT_OWN, 2048), BF16)
    x_ref[...] = jnp.zeros((DP, DP), F32)
    cacc[...] = jnp.zeros((DR, DP), F32)
    cov_out[...] = jnp.zeros(cov_out.shape, F32)
    t_nat[0] = t_all[0].T
    rmax[...] = jnp.full((8, 2048), -3e38, F32)
    rsum[...] = jnp.zeros((8, 2048), F32)
    pl.semaphore_wait(barrier, 8)

    def part(slot, half):
        return s_all.at[slot, pl.ds(HALVES[half][0], HALVES[half][1])]

    def s_hop(way, step, half):
        here = (8 - step) % 8 if way == 0 else step
        there = (here + 7) % 8 if way == 0 else here + 1
        to = (z + 1) % 8 if way == 0 else (z + 7) % 8
        return remote(
            part(2 * here, half), part(2 * there, half),
            s_send.at[way, step, half], s_recv.at[there, half], z_dev(to)
        )

    def s_wait(way, step, half):
        k = (8 - step) % 8 if way == 0 else step
        remote(part(2 * k, half), part(2 * k, half), s_send.at[0, 0, 0], s_recv.at[k, half], partner).wait_recv()

    def hand(k):
        return remote(s_all.at[2 * k], s_all.at[2 * k + 1], f_send.at[k], f_recv.at[k], partner)

    def handed(k):
        return remote(s_all.at[2 * k], s_all.at[2 * k + 1], f_send.at[0], f_recv.at[k], partner)

    def moved(i, j, to_i, to_j):
        return ((i - to_i) % 4) * 4 + (j - to_j) % 4

    def t_full(i, j, to_i, to_j, n):
        there = moved(i, j, to_i, to_j)
        return remote(
            t_all.at[4 * i + j], t_all.at[there], t_send.at[n], t_recv.at[there], t_dev(t_slot(to_i, to_j))
        )

    def t_half(i, j, half, to_i, to_j, n):
        there = moved(i, j, to_i, to_j)
        rows = pl.ds(HALVES[half][0], HALVES[half][1])
        return remote(
            t_all.at[4 * i + j, rows], t_all.at[there, rows],
            t_send.at[n], th_recv.at[there, half], t_dev(t_slot(to_i, to_j))
        )

    def t_wait(i, j):
        slot = 4 * i + j
        remote(t_all.at[slot], t_all.at[slot], t_send.at[0], t_recv.at[slot], partner).wait_recv()
        t_nat[slot] = t_all[slot].T

    def t_wait_halves(i, j):
        slot = 4 * i + j
        for half in range(2):
            ref = t_all.at[slot, pl.ds(HALVES[half][0], HALVES[half][1])]
            remote(ref, ref, t_send.at[0], th_recv.at[slot, half], partner).wait_recv()
        t_nat[slot] = t_all[slot].T

    sent = []

    def go(copy):
        copy.start()
        sent.append(copy)

    for half in range(2):
        go(s_hop(0, 0, half))
        go(s_hop(1, 0, half))
    go(t_full(0, 0, 1, 0, 0))
    go(t_full(0, 0, 3, 0, 1))
    go(t_full(0, 0, 0, 1, 2))
    go(t_full(0, 0, 0, 3, 3))
    go(t_full(0, 0, 2, 0, 4))
    go(hand(0))

    def s_stage(step):
        for half in range(2):
            for way in range(2):
                s_wait(way, step, half)
                if step < 3 or half == way:
                    go(s_hop(way, step, half))
        go(hand(8 - step))
        go(hand(step))

    def spread(i, n):
        go(t_full(i, 0, 0, 1, n))
        go(t_full(i, 0, 0, 3, n + 1))

    def spread_halves(i, n):
        t_wait(i, 3)
        go(t_half(i, 3, 0, 0, 1, n))
        t_wait(i, 1)
        go(t_half(i, 1, 1, 0, 3, n + 1))

    scale = 4.0 / math.sqrt(D) / LN2

    def tile(p, places):
        rhs = jnp.concatenate([s_all[2 * p], s_all[2 * p + 1]], axis=1)
        at = pl.ds(pl.multiple_of(p * 256, 256), 256)
        slots = [4 * i + j for i, j in places]
        m = rmax[:, at]
        total = rsum[:, at]
        for n in range(0, len(slots), 2):
            pair = slots[n:n + 2]
            v = nn(jnp.concatenate([t_nat[slot] for slot in pair], axis=0), rhs) * scale
            parts = []
            for k, slot in enumerate(pair):
                w = v[k * 128:k * 128 + 128]
                logit[slot * 128:slot * 128 + 128, at] = w
                parts.append(w[0:NT_OWN].reshape(NT_OWN // 8, 8, 256))
            w = jnp.concatenate(parts, axis=0)
            old = m
            m = jnp.maximum(old, jnp.max(w, axis=0))
            total = total * jnp.exp2(old - m) + jnp.sum(jnp.exp2(w - m[None]), axis=0)
        rmax[:, at] = m
        rsum[:, at] = total

    def tiles(first, n, places):
        for k in range(n):
            tile((first + k) % 8, places)

    first_five = ((0, 0), (1, 0), (3, 0), (0, 1), (0, 3))
    t_wait(3, 0)
    t_wait(1, 0)
    spread(3, 6)
    spread(1, 8)
    s_stage(1)
    t_wait(2, 0)
    spread(2, 12)
    spread_halves(0, 10)
    for k in (0, 1, 7):
        handed(k).wait_recv()
    tiles(7, 3, first_five)
    s_stage(2)
    spread_halves(3, 14)
    spread_halves(1, 16)
    ring = ((2, 0), (3, 3), (3, 1), (1, 3), (1, 1), (2, 3), (2, 1))
    last = ((0, 2), (1, 2), (2, 2), (3, 2))
    tiles(7, 3, ring[0:5])
    for k in (2, 6):
        handed(k).wait_recv()
        tile(k, first_five)
    s_stage(3)
    spread_halves(2, 18)
    for k in (2, 6):
        tile(k, ring)
    for k in (3, 5):
        handed(k).wait_recv()
        tile(k, first_five)
    tiles(7, 3, ring[5:])
    s_wait(0, 4, 0)
    s_wait(1, 4, 1)
    go(hand(4))
    tile(3, ring)
    tile(5, ring)
    for i in (0, 3, 1, 2):
        t_wait_halves(i, 2)
    for k in (3, 5, 2, 6, 1, 7, 0):
        tile(k, last)
    handed(4).wait_recv()
    tile(4, first_five + ring + last)

    def row_again():
        rsum[...] = jnp.zeros((8, 2048), F32)

        def block(b):
            rows = pl.ds(pl.multiple_of(b * 128, 128), NT_OWN)
            for j in range(16):
                cols = slice(j * 128, (j + 1) * 128)
                v = jnp.exp2(logit[rows, cols] + cexp[rows, :] + rrow[0:1, cols])
                logit[rows, cols] = v
                rsum[:, cols] += jnp.sum(v.reshape(NT_OWN // 8, 8, 128), axis=0)
        each(0, 16, block)

    def col_again():
        def block(b):
            rows = pl.ds(pl.multiple_of(b * 128, 128), NT_OWN)
            total = jnp.zeros((NT_OWN, 128), F32)
            for j in range(16):
                cols = slice(j * 128, (j + 1) * 128)
                total = total + logit[rows, cols] * rrow[0:1, cols]
            lsum[rows, :] = total
        each(0, 16, block)
        for i in range(NT_OWN // 8):
            column = jnp.zeros((8, 128), F32)
            for b in range(16):
                rows = slice(b * 128 + 8 * i, b * 128 + 8 * i + 8)
                column = jnp.where(lane == b, jnp.sum(lsum[rows, :], axis=1, keepdims=True), column)
            dense[8 * i:8 * i + 8, :] = column

    def col_pass():
        def block(b):
            for i in range(NT_OWN // 8):
                rows = pl.ds(pl.multiple_of(b * 128 + 8 * i, 8), 8)
                v = [
                    logit[rows, j * 128:(j + 1) * 128] + rrow[:, j * 128:(j + 1) * 128]
                    for j in range(16)
                ]
                m = v[0]
                for w in v[1:]:
                    m = jnp.maximum(m, w)
                total = jnp.exp2(v[0] - m)
                for w in v[1:]:
                    total = total + jnp.exp2(w - m)
                lmax[rows, :] = m
                lsum[rows, :] = total
        each(0, 16, block)
        for i in range(NT_OWN // 8):
            column = jnp.zeros((8, 128), F32)
            for b in range(16):
                rows = slice(b * 128 + 8 * i, b * 128 + 8 * i + 8)
                m = lmax[rows, :]
                top = jnp.max(m, axis=1, keepdims=True)
                whole = jnp.sum(lsum[rows, :] * jnp.exp2(m - top), axis=1, keepdims=True)
                column = jnp.where(lane == b, top + jnp.log2(whole), column)
            dense[8 * i:8 * i + 8, :] = column

    z_peers = [((z + k) % 8, z_dev((z + k) % 8)) for k in (4, 3, 5, 2, 6, 1, 7)]
    s_peers = []
    for k in (4, 3, 5, 2, 6, 1, 7, 0):
        for c in range(2):
            if k or c:
                slot = ((z + k) % 8) * 2 + (other if c else core)
                s_peers.append((slot, s_dev(slot)))
    t_peers = []
    for d in sorted(range(1, 16), key=lambda d: -(min(d // 4, 4 - d // 4) + min(d % 4, 4 - d % 4))):
        px, py = (x_hi * 2 + x_lo + d // 4) % 4, (y + d % 4) % 4
        t_peers.append((px * 4 + py, ((px // 2) * 8 + z, (px % 2) * 8 + py * 2 + core)))

    def exchange(out, into, send, recv, me, peers):
        for n, (slot, device) in enumerate(peers):
            remote(out, into.at[me], send.at[n], recv.at[me], device).start()
        into[pl.ds(me, 1)] = out[...][None]
        for n, (slot, device) in reversed(list(enumerate(peers))):
            copy = remote(out, into.at[slot], send.at[n], recv.at[slot], device)
            copy.wait_recv()
            copy.wait_send()

    def combined(into):
        a = into[...]
        m = jnp.max(a, axis=0)
        return -(m + jnp.log2(jnp.sum(jnp.exp2(a - m[None]), axis=0)))

    def s_order(r):
        return ((z + r // 2) % 8) * 2 + (core if r % 2 == 0 else other)

    def t_order(r):
        return t_slot(r // 4, r % 4)

    def to_rows(ref):
        for r in range(16):
            rrow[:, r * 128:(r + 1) * 128] = jnp.broadcast_to(ref[pl.ds(s_order(r), 1), :], (8, 128))

    def out_row(it, values):
        for r in range(16):
            row_out[it, pl.ds(s_order(r), 1), :] = values[:, r * 128:(r + 1) * 128]

    def out_col(it):
        lines[...] = dense[...].T[0:16, :]
        for r in range(16):
            col_out[it, pl.ds(t_order(r), 1), :] = lines[r:r + 1, :]

    def to_cols(ref):
        for r in range(16):
            dense[r:r + 1, :] = ref[pl.ds(t_order(r), 1), :]
        turned = dense[...].T
        for b in range(16):
            cexp[b * 128:(b + 1) * 128, :] = jnp.broadcast_to(turned[:, b:b + 1], (128, 128))

    top = jnp.max(rmax[...], axis=0, keepdims=True)
    whole = jnp.sum(rsum[...] * jnp.exp2(rmax[...] - top), axis=0, keepdims=True)
    out_row(0, top + jnp.log2(whole))
    exchange(row_out.at[0], row_in.at[0], row_send.at[0], row_recv.at[0], g, s_peers)
    rpot[...] = combined(row_in.at[0])
    to_rows(rpot)
    col_pass()
    out_col(0)
    exchange(col_out.at[0], col_in.at[0], col_send.at[0], col_recv.at[0], h, t_peers)
    cpot[...] = combined(col_in.at[0])
    to_cols(cpot)

    row_again()
    out_row(1, jnp.sum(rsum[...], axis=0, keepdims=True))
    exchange(row_out.at[1], row_in.at[1], row_send.at[1], row_recv.at[1], g, s_peers)
    whole = jnp.sum(row_in[1], axis=0)
    rpot[...] = rpot[...] - jnp.log2(whole)
    lines[...] = 1.0 / whole
    to_rows(lines)
    col_again()
    out_col(1)
    exchange(col_out.at[1], col_in.at[1], col_send.at[1], col_recv.at[1], h, t_peers)
    whole = jnp.sum(col_in[1], axis=0)
    cpot[...] = cpot[...] - jnp.log2(whole)
    lines[...] = 1.0 / whole
    to_cols(lines)

    rp_ref[...] = (rpot[pl.ds(g, 1), :] * LN2).reshape(128)
    cp_ref[...] = (cpot[pl.ds(h, 1), :] * LN2)[:, 0:NT_OWN].reshape(NT_OWN)

    def fill(q):
        for b in range(16):
            rows = slice(b * 128, b * 128 + NT_OWN)
            share = cexp[rows, :]
            for j in range(4):
                cols = slice(q * 512 + j * 128, q * 512 + j * 128 + 128)
                plan[rows, cols] = (logit[rows, cols] * rrow[0:1, cols] * share).astype(BF16)

    targets = jnp.concatenate([t_all[b] for b in range(16)], axis=1)
    fill(0)
    for q in range(4):
        if q < 3:
            fill(q + 1)
        piece = nn(targets, plan[:, q * 512:(q + 1) * 512])
        for j in range(4):
            summed[4 * q + j] = piece[:, j * 128:(j + 1) * 128]
        cacc[:, 0:DR] += nt(piece.astype(BF16), jnp.concatenate([s_all[4 * q + j] for j in range(4)], axis=1))

    for half in range(2):
        at = half * 152
        for r in range(19):
            for l in range(2):
                cov_out[half, l * 19 + r] = cacc[at + 8 * r:at + 8 * r + 8, l * 128:(l + 1) * 128]
        for r in range(10):
            last = cacc[at + 8 * r:at + 8 * r + 8, 256:384]
            if r < 9:
                last = last + pltpu.roll(cacc[at + 80 + 8 * r:at + 88 + 8 * r, 256:384], 64, 1)
            cov_out[half, 38 + r] = last
    cv = remote(cov_out.at[other], cov_pair, cv_send, cv_recv, partner)
    cv.start()

    pr = [
        remote(summed.at[2 * k + 1], pair_in.at[k], pair_send.at[k], pair_recv.at[k], partner) for k in range(8)
    ]

    cv.wait()
    for copy in pr:
        copy.start()
    rs_out[...] = (cov_out[pl.ds(core, 1)].reshape(48, 8, 128) + cov_pair[...]).reshape(16, 24, 128).astype(BF16)
    for n, (slot, device) in enumerate(t_peers):
        remote(rs_out.at[slot], rs_in.at[h], rs_send.at[n], rs_recv.at[h], device).start()
    rs_in[pl.ds(h, 1)] = rs_out[pl.ds(h, 1)]

    for k in range(1, 8):
        pr[k].wait_recv()
        z_out[k] = (summed[2 * k] + pair_in[k]).astype(BF16)

    for n, (slot, device) in reversed(list(enumerate(t_peers))):
        copy = remote(rs_out.at[slot], rs_in.at[slot], rs_send.at[n], rs_recv.at[slot], device)
        copy.wait_recv()
        copy.wait_send()
    zc_out[...] = jnp.sum(rs_in[...].astype(F32), axis=0).reshape(3, 8, 128)
    exchange(zc_out, zc_in, zc_send, zc_recv, z, z_peers)
    mine = jnp.sum(zc_in[...], axis=0)
    full[pl.ds(core, 1), pl.ds(h, 1)] = mine[None, None]

    for n, (slot, device) in enumerate(t_peers):
        remote(full.at[core, h], full.at[core, h], ag_send.at[n], ag_recv.at[h], device).start()

    def pass_on(slot):
        return remote(full.at[core, slot], full.at[core, slot], hf_send.at[slot], hf_recv.at[slot], partner)

    pass_on(h).start()

    def z_copy(k):
        return remote(z_out.at[k], z_in.at[k], z_send.at[k], z_recv.at[k], z_dev((z + k) % 8))
    each(1, 8, lambda k: z_copy(k).start())

    for n, (slot, device) in reversed(list(enumerate(t_peers))):
        copy = remote(full.at[core, slot], full.at[core, slot], ag_send.at[n], ag_recv.at[slot], device)
        copy.wait_recv()
        pass_on(slot).start()
        copy.wait_send()
    for slot in range(16):
        remote(full.at[other, slot], full.at[other, slot], hf_send.at[slot], hf_recv.at[slot], partner).wait_recv()

    def tile_of(half, t):
        return full[half, t // 3, t % 3]

    for half in range(2):
        at = half * 152
        for r in range(19):
            for l in range(2):
                x_ref[at + 8 * r:at + 8 * r + 8, l * 128:(l + 1) * 128] = tile_of(half, l * 19 + r)
        for r in range(10):
            last = tile_of(half, 38 + r)
            x_ref[at + 8 * r:at + 8 * r + 8, 256:384] = jnp.where(lane < 44, last, 0.0)
            if r < 9:
                x_ref[at + 80 + 8 * r:at + 88 + 8 * r, 256:384] = jnp.where(lane < 44, pltpu.roll(last, 64, 1), 0.0)

    cov = x_ref[...]
    square = jnp.sum(jnp.sum(cov * cov, axis=0, keepdims=True), axis=1, keepdims=True)
    x_ref[...] = cov / jnp.sqrt(square + 1e-06)
    eye = (
        lax.broadcasted_iota(jnp.int32, (DR, DP), 0) == lax.broadcasted_iota(jnp.int32, (DR, DP), 1)
    ).astype(F32)

    def newton_small(k):
        v = x_ref[0:DR, :]
        b = x_ref[...].astype(BF16)
        gram = nt(b[0:DR], b).astype(BF16)
        x_ref[0:DR, :] = 1.5 * v - 0.5 * nn(gram, b)

    def newton(k):
        v = x_ref[...]
        b = v.astype(BF16)
        rest = (0.5 * (eye - nt(b[0:DR], b))).astype(BF16)
        x_ref[0:DR, :] = v[0:DR] + nn(rest, b)

    def newton_exact(k):
        v = x_ref[...]
        hi, lo = split(v)
        gram = nt(hi[0:DR], hi) + (nt(hi[0:DR], lo) + nt(lo[0:DR], hi))
        rest_hi, rest_lo = split(0.5 * (eye - gram))
        x_ref[0:DR, :] = v[0:DR] + (nn(rest_hi, hi) + (nn(rest_hi, lo) + nn(rest_lo, hi)))

    each(0, SMALL_STEPS, newton_small)
    each(SMALL_STEPS, NEWTON - EXACT_STEPS, newton)
    each(0, EXACT_STEPS, newton_exact)

    ort_ref[...] = x_ref[...].T[0:D, 0:D]
    hi, lo = split(x_ref[0:DR, 0:DR])
    own = s_all[0]
    rot_ref[...] = (nn(hi, own) + nn(lo, own))[0:D, :].astype(BF16)

    each(1, 8, lambda k: z_copy(k).wait())
    pr[0].wait_recv()
    total = summed[0] + pair_in[0]
    for k in range(1, 8):
        total = total + z_in[k].astype(F32)
    mat_ref[...] = total[0:D, :]

    for copy in sent + pr:
        copy.wait_send()
    for slot in range(16):
        pass_on(slot).wait_send()


def store(*refs):
    for given, result in zip(refs[:5], refs[5:]):
        result[...] = given[...]


def body(source_words, target_words):
    dma = pltpu.SemaphoreType.DMA
    vmem = pl.BlockSpec(memory_space=pltpu.VMEM)
    results = pl.pallas_call(
        kernel,
        out_shape=(
            jax.ShapeDtypeStruct((D, 128), BF16),
            jax.ShapeDtypeStruct((D, 128), F32),
            jax.ShapeDtypeStruct((D, D), F32),
            jax.ShapeDtypeStruct((128,), F32),
            jax.ShapeDtypeStruct((NT_OWN,), F32),
        ),
        in_specs=[vmem, vmem],
        out_specs=(vmem,) * 5,
        scratch_shapes=[
            pltpu.VMEM((16, DR, 128), BF16),
            pltpu.VMEM((16, DR, 128), BF16),
            pltpu.VMEM((16, 128, DR), BF16),
            pltpu.VMEM((2048, 2048), F32),
            pltpu.VMEM((2048, 128), F32),
            pltpu.VMEM((8, 2048), F32),
            pltpu.VMEM((128, 128), F32),
            pltpu.VMEM((8, 2048), F32),
            pltpu.VMEM((8, 2048), F32),
            pltpu.VMEM((2048, 128), F32),
            pltpu.VMEM((2048, 128), F32),
            pltpu.VMEM((16, 128), F32),
            pltpu.VMEM((16, 128), F32),
            pltpu.VMEM((ITERS, 16, 128), F32),
            pltpu.VMEM((ITERS, 16, 16, 128), F32),
            pltpu.VMEM((ITERS, 16, 128), F32),
            pltpu.VMEM((ITERS, 16, 16, 128), F32),
            pltpu.VMEM((2048, 2048), BF16),
            pltpu.VMEM((16, 128), F32),
            pltpu.VMEM((16, DR, 128), F32),
            pltpu.VMEM((8, DR, 128), F32),
            pltpu.VMEM((8, DR, 128), BF16),
            pltpu.VMEM((8, DR, 128), BF16),
            pltpu.VMEM((DR, DP), F32),
            pltpu.VMEM((2, 48, 8, 128), F32),
            pltpu.VMEM((48, 8, 128), F32),
            pltpu.VMEM((16, 24, 128), BF16),
            pltpu.VMEM((16, 24, 128), BF16),
            pltpu.VMEM((3, 8, 128), F32),
            pltpu.VMEM((8, 3, 8, 128), F32),
            pltpu.VMEM((2, 16, 3, 8, 128), F32),
            pltpu.VMEM((DP, DP), F32),
            dma((2, 4, 2)), dma((8, 2)), dma((8,)), dma((8,)), dma((22,)), dma((16,)), dma((16, 2)),
            dma((ITERS, 16)), dma((ITERS, 16)), dma((ITERS, 16)), dma((ITERS, 16)),
            dma((8,)), dma((8,)), dma((8,)), dma((8,)), dma, dma, dma((16,)), dma((16,)),
            dma((8,)), dma((8,)), dma((16,)), dma((16,)), dma((16,)), dma((16,)),
        ],
        compiler_params=pltpu.CompilerParams(
            collective_id=0, has_side_effects=True, vmem_limit_bytes=60 * 1024 * 1024
        ),
    )(source_words.T, target_words.T)
    rot, mat, ort, rp, cp = pl.pallas_call(
        store,
        out_shape=tuple(jax.ShapeDtypeStruct(r.shape, r.dtype) for r in results),
        in_specs=[vmem] * 5,
        out_specs=(vmem,) * 5,
    )(*results)
    return rot.T, mat.T, ort, rp, cp


def solution(mesh):
    in_specs = (P(("src", "tgt"), None), P(("tgt", "src"), None))
    out_specs = (
        P(("src", "tgt"), None),
        P(("src", "tgt"), None),
        P(),
        P(("src", "tgt")),
        P(("tgt", "src")),
    )
    return jax.shard_map(body, mesh=mesh, in_specs=in_specs, out_specs=out_specs, check_vma=False)
```
